32 devices in a mesh: dp: 8 (over z, y), mp: 4 (over x, core).
Axes of the slice: x: 2, y: 2, z: 4, core: 2. Of those that a mesh axis runs over, the one named last changes fastest.
Arguments:
- queries: bfloat16 [128, 8192], P('dp', 'mp'), may hold values from -8 to 8
- incoming_key: bfloat16 [128, 1024], P('dp', 'mp'), may hold values from -4 to 4
- incoming_value: bfloat16 [128, 1024], P('dp', 'mp'), may hold values from -4 to 4
- key_cache: bfloat16 [256, 256, 1024], P('dp', None, 'mp'), may hold values from -8 to 8
- cached_values: bfloat16 [256, 256, 1024], P('dp', None, 'mp'), may hold values from -4 to 4
- task_key_scale: bfloat16 [256, 1024], P(None, 'mp'), may hold values from 0.099609375 to 1.8984375
- task_value_scale: bfloat16 [256, 1024], P(None, 'mp'), may hold values from 0.099609375 to 1.8984375
- out_weight: bfloat16 [8192, 8192], P('mp', 'dp'), may hold values from -0.0625 to 0.0625
- task_id: int32 [128], P('dp'), may hold values from 0 to 255, as said below
- cached_length: int32 [128], P('dp'), may hold values from 1 to 256, as said below
- task_owner: int32 [256], replicated, may hold values from 0 to 7, as said below
- cache_slot: int32 [128], P('dp'), may hold values from 0 to 31, as said below
Outputs:
- layer_out: bfloat16 [128, 8192], P('dp', 'mp')
The draws below stay inside these ranges and needn't reach their ends.
Inputs may be any that keep to these rules, and one draw needn't show every extreme that they name: `task_owner`: every dp index owns the same number of tasks. `task_id`: among the 16 requests of one dp index at most 4 have tasks of one owner; in every draw one owner gets exactly 4 from every dp index. `cache_slot`: requests of one owner have distinct slots; one owner uses all 32. `cached_length`: every dp index has a request with 256 cached positions.
All inputs are finite; a program needn't handle non-finite values.
Results may differ from the reference program's by a relative error of at most 0.0073.
Values may be sent and summed in bfloat16 or wider, within the bound.
A program may use at most 128 MiB of HBM per device.

```python
import math
import jax
import jax.numpy as jnp
from jax import lax

D = 8192
KEY_VALUE_HEADS = 8
HEAD_SIZE = 128
QUERY_HEADS = 64
TASK_TOTAL = 256
REQUESTS_PER_DP = 16
MAX_POSITIONS = 256
QUERY_PER_KV = 8
REQUEST_TOTAL = 128
CAP = 4
OWN_CAP = 32
CACHE_ROWS = 256
N_DP = 8


def routing(key):
    shuffle = jax.random.permutation(jax.random.fold_in(key, 11), TASK_TOTAL)
    task_owner = (shuffle % N_DP).astype(jnp.int32)
    hot_owner = jax.random.randint(jax.random.fold_in(key, 12), (), 0, N_DP)
    position = jnp.arange(REQUESTS_PER_DP)
    rotation = jax.random.randint(jax.random.fold_in(key, 13), (N_DP, 1), 0, N_DP - 1)
    others = (hot_owner + 1 + (position[None, :] - CAP + rotation) % (N_DP - 1)) % N_DP
    owners_block = jnp.where(position[None, :] < CAP, hot_owner, others)
    block_keys = jax.random.split(jax.random.fold_in(key, 14), N_DP)
    orders = jax.vmap(lambda one_key: jax.random.permutation(one_key, REQUESTS_PER_DP))(block_keys)
    owners = jnp.take_along_axis(owners_block, orders, axis=1).reshape(REQUEST_TOTAL)
    within = jax.random.randint(jax.random.fold_in(key, 15), (REQUEST_TOTAL,), 0, TASK_TOTAL // N_DP)
    inverse = jnp.argsort(shuffle)
    task_id = inverse[owners + N_DP * within].astype(jnp.int32)
    mixing = jax.random.permutation(jax.random.fold_in(key, 16), REQUEST_TOTAL)
    ranking = jnp.argsort(owners * REQUEST_TOTAL + mixing)
    sorted_owner = owners[ranking]
    counts = jnp.sum((sorted_owner[:, None] == jnp.arange(N_DP)[None, :]).astype(jnp.int32), axis=0)
    starts = jnp.cumsum(counts) - counts
    rank_sorted = jnp.arange(REQUEST_TOTAL) - starts[sorted_owner]
    cache_slot = jnp.zeros((REQUEST_TOTAL,), jnp.int32).at[ranking].set(rank_sorted.astype(jnp.int32))
    return (task_owner, task_id, cache_slot)


def draw_task_owner(key, part):
    return routing(key)[0]


def draw_task_id(key, part):
    return routing(key)[1]


def draw_cache_slot(key, part):
    return routing(key)[2]


def draw_cached_length(key, part):
    lengths = jax.random.randint(jax.random.fold_in(key, 21), (N_DP, REQUESTS_PER_DP), 1, MAX_POSITIONS + 1)
    longest = jax.random.randint(jax.random.fold_in(key, 22), (N_DP, 1), 0, REQUESTS_PER_DP)
    lengths = jnp.where(jnp.arange(REQUESTS_PER_DP)[None, :] == longest, MAX_POSITIONS, lengths)
    return lengths.reshape(REQUEST_TOTAL).astype(jnp.int32)


def draw_queries(key, part):
    random_noise = jax.random.normal(jax.random.fold_in(key, 32), (REQUEST_TOTAL, QUERY_HEADS * HEAD_SIZE), jnp.float32)
    value_rows = jnp.clip(2.0 * random_noise, -6.0, 6.0)
    return value_rows.astype(jnp.bfloat16)


def draw_key_cache(key, part):
    random_noise = jax.random.normal(jax.random.fold_in(key, 33), (CACHE_ROWS, MAX_POSITIONS, KEY_VALUE_HEADS * HEAD_SIZE), jnp.float32)
    value_rows = jnp.clip(random_noise, -4.0, 4.0)
    return value_rows.astype(jnp.bfloat16)


def block_levels(key, dims, cuts, least, top_value):
    loudness, own = 1.0, jax.random.fold_in(key, 6)
    for dim, shards_of in cuts:
        draws = jnp.exp(jax.random.uniform(jax.random.fold_in(own, dim), (shards_of,), jnp.float32, least / len(cuts), top_value / len(cuts)))
        loudness = loudness * jnp.repeat(draws, dims[dim] // shards_of).reshape([-1 if axis == dim else 1 for axis in range(len(dims))])
    return loudness


def normal_values(stream_key, shape, scale, most, pieces=(), kind=jnp.bfloat16):
    values = jax.random.normal(stream_key, shape, jnp.float32) * scale
    if len(pieces) > 0:
        values = block_levels(stream_key, shape, pieces, -0.22, 0.18) * values
    return jnp.clip(values, min=-most, max=most).astype(kind)


def setup_inputs(seed: int = 0) -> dict:
    streams_of = jax.random.split(jax.random.key(seed), 13)
    return {
        "queries": draw_queries(jax.random.fold_in(streams_of[12], 71), 0),
        "incoming_key": normal_values(streams_of[1], (REQUEST_TOTAL, KEY_VALUE_HEADS * HEAD_SIZE), 1.0, 4.0, ((0, 8), (1, 4))),
        "incoming_value": normal_values(streams_of[2], (REQUEST_TOTAL, KEY_VALUE_HEADS * HEAD_SIZE), 1.0, 4.0, ((0, 8), (1, 4))),
        "key_cache": draw_key_cache(jax.random.fold_in(streams_of[12], 71), 0),
        "cached_values": normal_values(streams_of[4], (CACHE_ROWS, MAX_POSITIONS, KEY_VALUE_HEADS * HEAD_SIZE), 1.0, 4.0, ((0, 8), (2, 4))),
        "task_key_scale": jnp.clip(1.0 + 0.18 * jax.random.normal(streams_of[5], (TASK_TOTAL, KEY_VALUE_HEADS * HEAD_SIZE), jnp.float32), 0.099609375, 1.8984375).astype(jnp.bfloat16),
        "task_value_scale": jnp.clip(1.0 + 0.18 * jax.random.normal(streams_of[6], (TASK_TOTAL, KEY_VALUE_HEADS * HEAD_SIZE), jnp.float32), 0.099609375, 1.8984375).astype(jnp.bfloat16),
        "out_weight": normal_values(streams_of[7], (QUERY_HEADS * HEAD_SIZE, D), (QUERY_HEADS * HEAD_SIZE) ** -0.5, 0.0625, ((0, 4), (1, 8))),
        "task_id": draw_task_id(jax.random.fold_in(streams_of[12], 71), 0),
        "cached_length": draw_cached_length(jax.random.fold_in(streams_of[12], 71), 0),
        "task_owner": draw_task_owner(jax.random.fold_in(streams_of[12], 71), 0),
        "cache_slot": draw_cache_slot(jax.random.fold_in(streams_of[12], 71), 0),
    }


masked_score = -1e+30

def lowered_program(value_rows):
    return lax.optimization_barrier(value_rows.astype(jnp.bfloat16))

def attend(queries, fresh_key_rows, fresh_value_rows, stored_key_rows, stored_value_rows, lengths):
    entry_count = queries.shape[0]
    inv_root = 1.0 / math.sqrt(HEAD_SIZE)
    query_head_rows = queries.astype(jnp.float32).reshape(entry_count, KEY_VALUE_HEADS, QUERY_PER_KV, HEAD_SIZE)
    previous_keys = stored_key_rows.astype(jnp.float32).reshape(entry_count, MAX_POSITIONS, KEY_VALUE_HEADS, HEAD_SIZE)
    previous_values = stored_value_rows.astype(jnp.float32).reshape(entry_count, MAX_POSITIONS, KEY_VALUE_HEADS, HEAD_SIZE)
    incoming_keys = fresh_key_rows.astype(jnp.float32).reshape(entry_count, KEY_VALUE_HEADS, HEAD_SIZE)
    incoming_values = fresh_value_rows.astype(jnp.float32).reshape(entry_count, KEY_VALUE_HEADS, HEAD_SIZE)
    scores = jnp.einsum('ngqd,njgd->ngqj', query_head_rows, previous_keys, precision=lax.Precision.HIGHEST) * inv_root
    own_score = jnp.einsum('ngqd,ngd->ngq', query_head_rows, incoming_keys, precision=lax.Precision.HIGHEST) * inv_root
    visible = jnp.arange(MAX_POSITIONS)[None, None, None, :] < lengths[:, None, None, None]
    scores = jnp.where(visible, scores, masked_score)
    top_score = jnp.maximum(lax.optimization_barrier(jnp.max(scores, axis=3)), own_score)
    weights = jnp.where(visible, jnp.exp(scores - top_score[..., None]), 0.0)
    own_weight = jnp.exp(own_score - top_score)
    weight_sum = lax.optimization_barrier(jnp.sum(weights, axis=3)) + own_weight
    blended = jnp.einsum('ngqj,njgd->ngqd', lowered_program(weights).astype(jnp.float32), previous_values, precision=lax.Precision.HIGHEST)
    blended = blended + lowered_program(own_weight).astype(jnp.float32)[..., None] * incoming_values[:, :, None, :]
    return (blended / weight_sum[..., None]).astype(jnp.bfloat16).reshape(entry_count, QUERY_HEADS * HEAD_SIZE)

def reference(queries, incoming_key, incoming_value, key_cache, cached_values, task_key_scale, task_value_scale, out_weight, task_id, cached_length, task_owner, cache_slot):
    owner_of = jnp.take(task_owner, task_id).astype(jnp.int32)
    owner_row_index = (owner_of * OWN_CAP + cache_slot).astype(jnp.int32)
    key_factor = jnp.take(task_key_scale, task_id, axis=0).astype(jnp.float32)
    value_factor = jnp.take(task_value_scale, task_id, axis=0).astype(jnp.float32)
    scaled_rows = lowered_program((queries.astype(jnp.float32).reshape(REQUEST_TOTAL, KEY_VALUE_HEADS, QUERY_PER_KV, HEAD_SIZE) * key_factor.reshape(REQUEST_TOTAL, KEY_VALUE_HEADS, 1, HEAD_SIZE)).reshape(REQUEST_TOTAL, QUERY_HEADS * HEAD_SIZE))

    def block_kernel(members):
        block_queries, block_keys, block_values, block_rows, block_lengths = members
        stored_key_rows = jnp.take(key_cache, block_rows, axis=0)
        stored_value_rows = jnp.take(cached_values, block_rows, axis=0)
        return attend(block_queries, block_keys, block_values, stored_key_rows, stored_value_rows, block_lengths)
    attention_output = lax.map(block_kernel, (scaled_rows.reshape(N_DP, REQUESTS_PER_DP, QUERY_HEADS * HEAD_SIZE), incoming_key.reshape(N_DP, REQUESTS_PER_DP, KEY_VALUE_HEADS * HEAD_SIZE), incoming_value.reshape(N_DP, REQUESTS_PER_DP, KEY_VALUE_HEADS * HEAD_SIZE), owner_row_index.reshape(N_DP, REQUESTS_PER_DP), cached_length.reshape(N_DP, REQUESTS_PER_DP)))
    attention_output = attention_output.reshape(REQUEST_TOTAL, QUERY_HEADS * HEAD_SIZE)
    context_rows = lowered_program((attention_output.astype(jnp.float32).reshape(REQUEST_TOTAL, KEY_VALUE_HEADS, QUERY_PER_KV, HEAD_SIZE) * value_factor.reshape(REQUEST_TOTAL, KEY_VALUE_HEADS, 1, HEAD_SIZE)).reshape(REQUEST_TOTAL, QUERY_HEADS * HEAD_SIZE))
    return jnp.dot(context_rows, out_weight, preferred_element_type=jnp.float32).astype(jnp.bfloat16)
```

```python
import contextlib
import functools
import math

import jax
import jax.numpy as jnp
from jax import lax
from jax.experimental import pallas as pl
from jax.experimental.pallas import tpu as pltpu
from jax.sharding import PartitionSpec as P

KEY_VALUE_HEADS = 8
HEAD_SIZE = 128
QUERY_HEADS = 64
GROUP = QUERY_HEADS // KEY_VALUE_HEADS
META = 128
FIRST = 16
SUBS = 2
SIDE = 2
SCOPES = False
MESH = pl.DeviceIdType.MESH

masked_score = -1e30
f32 = jnp.float32
bf16 = jnp.bfloat16


def phase(name):
    return jax.named_scope(name) if SCOPES else contextlib.nullcontext()


def iota(shape, dim):
    return lax.broadcasted_iota(jnp.int32, shape, dim)


def to_column(row):
    n = row.shape[1]
    eye = iota((n, n), 0) == iota((n, n), 1)
    return jnp.sum(jnp.where(eye, row, 0.0), axis=1, keepdims=True)


def to_row(column):
    n = column.shape[0]
    eye = iota((n, n), 0) == iota((n, n), 1)
    return jnp.sum(jnp.where(eye, column, 0.0), axis=0, keepdims=True)


def factors(dp):
    inner = 2 ** (int(math.log2(dp)) // 2)
    return dp // inner, inner


def dot(a, b):
    return jnp.dot(a, b, preferred_element_type=f32)


def pick(table, index):
    value = table[0]
    for i in range(1, len(table)):
        value = jnp.where(index == i, table[i], value)
    return value


def far_first(count):
    return [sorted(range(count), key=lambda t: -abs(t - z)) for z in range(count)]


def relays(z, source, count):
    beyond = z + (1 if z > source else -1)
    return abs(z - source) >= 2 and 0 <= beyond < count


def arrival_order(count):
    def rank(z):
        return lambda s: abs(z - s) - (1.5 if relays(z, s, count) else 0.0)

    return [sorted((s for s in range(count) if s != z), key=rank(z)) for z in range(count)]


def layer_kernel(
    dp,
    mp,
    query_hbm,
    new_key_hbm,
    new_value_hbm,
    key_scale_hbm,
    value_scale_hbm,
    task_hbm,
    length_hbm,
    slot_hbm,
    owner_hbm,
    key_hbm,
    value_hbm,
    weight_hbm,
    out_ref,
    query_ref,
    new_key_ref,
    new_value_ref,
    key_scale_ref,
    value_scale_ref,
    task_ref,
    length_ref,
    slot_ref,
    owner_ref,
    keys,
    values,
    weight,
    rows_f32,
    in_f32,
    fact_rows,
    send_rows,
    recv_rows,
    pair_query,
    pair_small,
    value_scale,
    slot_length,
    slot_context,
    context,
    selector,
    total,
    give,
    take,
    send_part,
    recv_part,
    input_sem,
    fetch_sem,
    request_send,
    request_recv,
    along_send,
    along_recv,
    relay_send,
    across_send,
    across_recv,
    side_send,
    swap_sem,
    part_send,
    part_recv,
):
    me = lax.axis_index("dp")
    part = lax.axis_index("mp")
    rows, query_width = query_ref.shape
    groups = new_key_ref.shape[1] // HEAD_SIZE
    group_width = GROUP * HEAD_SIZE
    segment = group_width + 2 * HEAD_SIZE
    task_total = key_scale_ref.shape[0]
    slots, positions, _ = keys.shape
    capacity = send_rows.shape[1]
    items = dp * capacity
    columns = 2 * weight.shape[2]
    blocks = dp // mp
    half = slots // 2
    per = half // SUBS
    outer, inner = factors(dp)
    z, y = me // inner, lax.rem(me, inner)

    barrier = pltpu.get_barrier_semaphore()
    for k in range(1, dp):
        pl.semaphore_signal(
            barrier, inc=1, device_id=(lax.rem(me + k, dp), part), device_id_type=MESH
        )
    for k in range(1, mp):
        pl.semaphore_signal(
            barrier, inc=1, device_id=(me, lax.rem(part + k, mp)), device_id_type=MESH
        )

    pairs = [
        (task_hbm, task_ref),
        (owner_hbm, owner_ref),
        (length_hbm, length_ref),
        (slot_hbm, slot_ref),
        (key_scale_hbm, key_scale_ref),
        (query_hbm, query_ref),
        (new_key_hbm, new_key_ref),
        (new_value_hbm, new_value_ref),
        (value_scale_hbm, value_scale_ref),
    ]
    inputs = [pltpu.make_async_copy(a, b, input_sem.at[i]) for i, (a, b) in enumerate(pairs)]
    for copy in inputs:
        copy.start()
    parity = lax.rem(part, 2)
    width = weight.shape[2]
    kept_lanes = pl.ds(pl.multiple_of(parity * width, width), width)
    given_lanes = pl.ds(pl.multiple_of((1 - parity) * width, width), width)
    fetches = [
        pltpu.make_async_copy(key_hbm, keys, fetch_sem.at[0]),
        pltpu.make_async_copy(value_hbm, values, fetch_sem.at[1]),
        pltpu.make_async_copy(weight_hbm.at[:, given_lanes], weight.at[0], fetch_sem.at[2]),
        pltpu.make_async_copy(weight_hbm.at[:, kept_lanes], weight.at[1], fetch_sem.at[3]),
    ]
    pair_query[...] = jnp.zeros_like(pair_query)

    def start_of(g):
        return g * segment + (META if g > 0 else 0)

    def span_of(g):
        return slice(start_of(g), start_of(g) + segment + (META if g == 0 else 0))

    meta = slice(segment, segment + META)

    with phase("inputs"):
        for copy in inputs[:4]:
            copy.wait()
    with phase("pack0"):
        task_column = to_column(task_ref[...].astype(f32))
        length_column = to_column(length_ref[...].astype(f32))
        slot_column = to_column(slot_ref[...].astype(f32))
        picked = task_column == iota((rows, task_total), 1).astype(f32)
        owner_column = jnp.sum(
            jnp.where(picked, owner_ref[...].astype(f32), 0.0), axis=1, keepdims=True
        )
        owner_row = to_row(owner_column)
        earlier = iota((rows, rows), 1) < iota((rows, rows), 0)
        rank = jnp.sum(
            jnp.where(earlier & (owner_column == owner_row), 1.0, 0.0), axis=1, keepdims=True
        )
        position_row = to_row(owner_column * capacity + rank)
        packer = jnp.where(
            position_row == iota((items, rows), 0).astype(f32), 1.0, 0.0
        ).astype(bf16)
        side = jnp.floor(slot_column * (1.0 / half))
        pair = slot_column - side * half
        sub = jnp.floor(pair * (1.0 / per))
        line_column = sub * (2 * per) + side * per + (pair - sub * per)
        lane = iota((rows, META), 1)
        line = iota((rows, META), 0)
        task_high = jnp.floor(task_column * (1.0 / 128.0))
        task_low = task_column - task_high * 128.0
        facts = (
            jnp.where(lane == 0, slot_column + 1.0, 0.0)
            + jnp.where(lane == 1, length_column, 0.0)
            + jnp.where(lane == 2, task_high, 0.0)
            + jnp.where(lane == 3, task_low, 0.0)
        )
        shared = jnp.sum(
            jnp.where(lane == FIRST + line, owner_column, 0.0)
            + jnp.where(lane == FIRST + rows + line, line_column, 0.0),
            axis=0,
            keepdims=True,
        )
        rows_f32[:, meta] = dot(packer, facts.astype(bf16)) + shared
        for copy in inputs[4:]:
            copy.wait()
        for fetch in fetches:
            fetch.start()
        key_factor = dot(jnp.where(picked, 1.0, 0.0).astype(bf16), key_scale_ref[...])

    def pack(g):
        own = slice(g * HEAD_SIZE, (g + 1) * HEAD_SIZE)
        at = start_of(g)
        for h in range(GROUP):
            lanes = slice((g * GROUP + h) * HEAD_SIZE, (g * GROUP + h + 1) * HEAD_SIZE)
            scaled = (query_ref[:, lanes].astype(f32) * key_factor[:, own]).astype(bf16)
            rows_f32[:, at + h * HEAD_SIZE : at + (h + 1) * HEAD_SIZE] = dot(packer, scaled)
        first = key_at(g)
        rows_f32[:, first : first + HEAD_SIZE] = dot(packer, new_key_ref[:, own])
        rows_f32[:, first + HEAD_SIZE : first + 2 * HEAD_SIZE] = dot(packer, new_value_ref[:, own])
        for d in range(dp):
            send_rows[d, :, span_of(g)] = rows_f32[
                d * capacity : (d + 1) * capacity, span_of(g)
            ].astype(bf16)

    def key_at(g):
        return start_of(g) + group_width

    far = far_first(outer)
    sends = [(i, j) for i in range(outer) for j in range(inner - 1, -1, -1)][:-1]

    def request_copy(g, i, j):
        target = pick([far[t][i] for t in range(outer)], z) * inner + lax.rem(y + j, inner)
        return pltpu.make_async_remote_copy(
            src_ref=send_rows.at[target, :, span_of(g)],
            dst_ref=recv_rows.at[me, :, span_of(g)],
            send_sem=request_send.at[g, i * inner + j],
            recv_sem=request_recv.at[g, me],
            device_id=(target, part),
            device_id_type=MESH,
        )

    def request_arrival(g, k):
        source = lax.rem(me + k, dp)
        return pltpu.make_async_remote_copy(
            src_ref=send_rows.at[0, :, span_of(g)],
            dst_ref=recv_rows.at[source, :, span_of(g)],
            send_sem=request_send.at[g, 0],
            recv_sem=request_recv.at[g, source],
            device_id=(source, part),
            device_id_type=MESH,
        )

    with phase("pack1"):
        pack(0)
    with phase("barrier"):
        pl.semaphore_wait(barrier, dp + mp - 2)
    for g in range(groups):
        if g > 0:
            with phase("pack2"):
                pack(g)
        for i, j in sends:
            request_copy(g, i, j).start()
    recv_rows[me] = send_rows[me]

    inv_root = 1.0 / math.sqrt(HEAD_SIZE)
    key_line = iota((2 * GROUP, positions), 1).astype(f32)
    low_line = iota((2 * GROUP, positions), 0) < GROUP

    def attend(g, sub):
        own = slice(g * HEAD_SIZE, (g + 1) * HEAD_SIZE)
        picks = [sub * per + i for i in range(per)]

        def both(ref, p):
            return jnp.concatenate([ref[p, :, own], ref[p + half, :, own]], axis=1)

        scores, owns, weights, own_weights, tops, shows, sees = [], [], [], [], [], [], []
        for p in picks:
            scores.append(
                lax.dot_general(
                    pair_query[p].astype(bf16),
                    both(keys, p),
                    (((1,), (1,)), ((), ())),
                    preferred_element_type=f32,
                )
                * inv_root
            )
        for p in picks:
            owns.append(
                jnp.sum(pair_query[p] * pair_small[0, p : p + 1, :], axis=1, keepdims=True)
                * inv_root
            )
        for i, p in enumerate(picks):
            length = jnp.where(
                low_line, slot_length[p : p + 1, :], slot_length[p + half : p + half + 1, :]
            )
            sees.append(key_line < length)
            shows.append(jnp.where(sees[i], scores[i], masked_score))
            tops.append(jnp.maximum(jnp.max(shows[i], axis=1, keepdims=True), owns[i]))
        for i in range(per):
            weights.append(jnp.where(sees[i], jnp.exp(shows[i] - tops[i]), 0.0))
            own_weights.append(jnp.exp(owns[i] - tops[i]))
        blends = [dot(weights[i].astype(bf16), both(values, p)) for i, p in enumerate(picks)]
        for i, p in enumerate(picks):
            weight_sum = jnp.sum(weights[i], axis=1, keepdims=True) + own_weights[i]
            one = slice(p, p + 1)
            blended = blends[i] + own_weights[i].astype(bf16).astype(f32) * pair_small[1, one, :]
            attended = (blended / weight_sum).astype(bf16).astype(f32) * pair_small[2, one, :]
            slot_context[i, :GROUP, :] = attended[:GROUP, :HEAD_SIZE]
            slot_context[i, GROUP:, :] = attended[GROUP:, HEAD_SIZE:]
        for h in range(GROUP):
            context[g, me, sub, :, h * HEAD_SIZE : (h + 1) * HEAD_SIZE] = jnp.concatenate(
                [slot_context[:, h, :], slot_context[:, GROUP + h, :]], axis=0
            ).astype(bf16)

    def near_copy(g, sub, target):
        return pltpu.make_async_remote_copy(
            src_ref=context.at[g, me, sub],
            dst_ref=context.at[g, me, sub],
            send_sem=along_send.at[target, g, sub],
            recv_sem=along_recv.at[z, g, sub],
            device_id=(target * inner + y, part),
            device_id_type=MESH,
        )

    def is_near(target):
        return (target != z) & (target - z < 3) & (z - target < 3)

    def along_arrival(g, sub, source):
        at = source * inner + y
        return pltpu.make_async_remote_copy(
            src_ref=context.at[g, at, sub],
            dst_ref=context.at[g, at, sub],
            send_sem=along_send.at[0, g, sub],
            recv_sem=along_recv.at[source, g, sub],
            device_id=(at, part),
            device_id_type=MESH,
        )

    def relay_copy(g, sub, source):
        at = source * inner + y
        beyond = z + jnp.where(z > source, 1, -1)
        return pltpu.make_async_remote_copy(
            src_ref=context.at[g, at, sub],
            dst_ref=context.at[g, at, sub],
            send_sem=relay_send.at[source, g, sub],
            recv_sem=along_recv.at[source, g, sub],
            device_id=(beyond * inner + y, part),
            device_id_type=MESH,
        )

    def is_relay(source):
        up = (z - source >= 2) & (z < outer - 1)
        down = (source - z >= 2) & (z > 0)
        return up | down

    def across_copy(g, sub, source, j):
        at = source * inner + y
        return pltpu.make_async_remote_copy(
            src_ref=context.at[g, at, sub],
            dst_ref=context.at[g, at, sub],
            send_sem=across_send.at[source, j, g, sub],
            recv_sem=across_recv.at[at, g, sub],
            device_id=(z * inner + lax.rem(y + j, inner), part),
            device_id_type=MESH,
        )

    def across_arrival(g, sub, source, j):
        at = source * inner + lax.rem(y + j, inner)
        return pltpu.make_async_remote_copy(
            src_ref=context.at[g, at, sub],
            dst_ref=context.at[g, at, sub],
            send_sem=across_send.at[0, 0, g, sub],
            recv_sem=across_recv.at[at, g, sub],
            device_id=(at, part),
            device_id_type=MESH,
        )

    chunks = [(g, sub) for g in range(groups) for sub in range(SUBS)]
    side_chunks = SIDE * len(chunks) // 4
    for g in range(groups):
        with phase("requests"):
            for k in range(1, dp):
                request_arrival(g, k).wait_recv()
        with phase("place"):
            for s in range(dp):
                in_f32[s * capacity : (s + 1) * capacity, span_of(g)] = recv_rows[
                    s, :, span_of(g)
                ].astype(f32)
            if g == 0:
                facts_in = in_f32[:, meta]
                for s in range(dp):
                    fact_rows[s] = in_f32[s * capacity : s * capacity + 1, meta]
                placing_row = to_row(facts_in[:, 0:1])
                placer = jnp.where(
                    placing_row == iota((slots, items), 0).astype(f32) + 1.0, 1.0, 0.0
                ).astype(bf16)
                slot_facts = dot(placer, facts_in.astype(bf16))
                slot_task = slot_facts[:, 2:3] * 128.0 + slot_facts[:, 3:4]
                value_scale[...] = dot(
                    jnp.where(slot_task == iota((slots, task_total), 1).astype(f32), 1.0, 0.0).astype(bf16),
                    value_scale_ref[...],
                )
                slot_length[...] = jnp.broadcast_to(slot_facts[:, 1:2], (slots, positions))
            at = start_of(g)
            for h in range(GROUP):
                placed = dot(
                    placer, in_f32[:, at + h * HEAD_SIZE : at + (h + 1) * HEAD_SIZE].astype(bf16)
                )
                pair_query[:, h, :HEAD_SIZE] = placed[:half]
                pair_query[:, GROUP + h, HEAD_SIZE:] = placed[half:]
            for i in range(2):
                first = key_at(g) + i * HEAD_SIZE
                small = dot(placer, in_f32[:, first : first + HEAD_SIZE].astype(bf16))
                pair_small[i, :, :HEAD_SIZE] = small[:half]
                pair_small[i, :, HEAD_SIZE:] = small[half:]
            own = slice(g * HEAD_SIZE, (g + 1) * HEAD_SIZE)
            pair_small[2, :, :HEAD_SIZE] = value_scale[:half, own]
            pair_small[2, :, HEAD_SIZE:] = value_scale[half:, own]
        if g == 0:
            with phase("fetch"):
                fetches[0].wait()
                fetches[1].wait()
        for sub in range(SUBS):
            with phase("attend"):
                attend(g, sub)
            for j in range(1, inner):
                across_copy(g, sub, z, j).start()
            for i in range(outer - 1):
                target = pick([far[t][i] for t in range(outer)], z)

                @pl.when(is_near(target))
                def _():
                    near_copy(g, sub, target).start()

    with phase("selector"):
        lane_r = iota((rows, META), 1)
        line_r = iota((rows, META), 0)
        for i in range(dp):
            fact_row = fact_rows[i]
            owner_in = jnp.sum(
                jnp.where(lane_r == FIRST + line_r, fact_row, 0.0), axis=1, keepdims=True
            )
            line_in = jnp.sum(
                jnp.where(lane_r == FIRST + rows + line_r, fact_row, 0.0), axis=1, keepdims=True
            )
            selector[i * rows : (i + 1) * rows, :] = jnp.where(
                owner_in * slots + line_in == iota((rows, dp * slots), 1).astype(f32), 1.0, 0.0
            ).astype(bf16)

    beside = z + 1 - 2 * lax.rem(z, 2)

    def side_copy(g, sub, j):
        at = z * inner + lax.rem(y + j, inner)
        return pltpu.make_async_remote_copy(
            src_ref=context.at[g, at, sub],
            dst_ref=context.at[g, at, sub],
            send_sem=side_send.at[j, g, sub],
            recv_sem=across_recv.at[at, g, sub],
            device_id=(beside * inner + y, part),
            device_id_type=MESH,
        )

    order = arrival_order(outer)
    late = outer - 2
    events = sorted(
        [(c + (1.5 if r >= late else 0.0), r, c) for c in range(len(chunks)) for r in range(outer - 1)]
        + [(c - 0.5, -1, c) for c in range(side_chunks)]
    )
    with phase("forward"):
        for _, r, c in events:
            g, sub = chunks[c]
            if r < 0:
                for j in range(1, inner):
                    across_arrival(g, sub, z, j).wait_recv()
                    side_copy(g, sub, j).start()
                continue
            source = pick([order[t][r] for t in range(outer)], z)
            along_arrival(g, sub, source).wait_recv()

            @pl.when(is_relay(source))
            def _():
                relay_copy(g, sub, source).start()

            if c < side_chunks:

                @pl.when(source != beside)
                def _():
                    for j in range(1, inner):
                        across_copy(g, sub, source, j).start()

            else:
                for j in range(1, inner):
                    across_copy(g, sub, source, j).start()

    fetches[2].wait()
    fetches[3].wait()

    def arrange(g):
        blocks_of = context[g].reshape(dp * slots, group_width)
        return dot(selector[...], blocks_of).astype(bf16)

    def product(arranged, g, n):
        found = dot(arranged, weight[n, g * group_width : (g + 1) * group_width, :])
        return found.reshape(dp, rows, width)

    def gathered(g):
        for sub in range(SUBS):
            for i in range(outer):
                if i == outer - 1 and chunks.index((g, sub)) < side_chunks:
                    continue
                source = pick([order[t][i] if i < outer - 1 else t for t in range(outer)], z)
                for j in range(1, inner):
                    across_arrival(g, sub, source, j).wait_recv()

    for g in range(groups - 1):
        with phase("across"):
            gathered(g)
        with phase("product"):
            arranged = arrange(g)
            for n in range(2):
                found = product(arranged, g, n)
                total[n] = found if g == 0 else total[n] + found
    with phase("across"):
        gathered(groups - 1)

    partner = part + 1 - 2 * parity
    swap = pltpu.make_async_remote_copy(
        src_ref=give,
        dst_ref=take,
        send_sem=swap_sem.at[0],
        recv_sem=swap_sem.at[1],
        device_id=(me, partner),
        device_id_type=MESH,
    )
    with phase("product"):
        arranged = arrange(groups - 1)
        given = product(arranged, groups - 1, 0)
        give[...] = (given if groups == 1 else given + total[0]).astype(bf16)
    swap.start()
    with phase("product"):
        kept = product(arranged, groups - 1, 1)
        total[1] = kept if groups == 1 else kept + total[1]
    with phase("swap"):
        swap.wait_recv()

    target_part = me // blocks
    place = lax.rem(me, blocks) * mp + part

    def part_target(i, j):
        return pick([far[t][i] for t in range(outer)], z) * inner + lax.rem(y + j, inner)

    def part_copy(i, j):
        target = part_target(i, j)
        return pltpu.make_async_remote_copy(
            src_ref=send_part.at[target],
            dst_ref=recv_part.at[place],
            send_sem=part_send.at[target],
            recv_sem=part_recv.at[place],
            device_id=(target, target_part),
            device_id_type=MESH,
        )
    def part_arrival(j):
        return pltpu.make_async_remote_copy(
            src_ref=send_part.at[0],
            dst_ref=recv_part.at[j],
            send_sem=part_send.at[0],
            recv_sem=part_recv.at[j],
            device_id=(me, part),
            device_id_type=MESH,
        )

    with phase("parts"):
        for i, j in sends + [(outer - 1, 0)]:
            target = part_target(i, j)
            send_part[target] = (total[1, target] + take[target].astype(f32)).astype(bf16)
            if (i, j) in sends:
                part_copy(i, j).start()

        @pl.when(target_part != part)
        def _():
            part_copy(outer - 1, 0).start()

        @pl.when(target_part == part)
        def _():
            recv_part[place] = send_part[me]

        for j in range(blocks * mp):
            stays = (part * blocks + j // mp == me) & (part == j % mp)

            @pl.when(jnp.logical_not(stays))
            def _():
                part_arrival(j).wait_recv()

    for e in range(blocks):
        for n in range(2):
            summed = recv_part[e * mp + n].astype(f32)
            for j in range(n + 2, mp, 2):
                summed = summed + recv_part[e * mp + j].astype(f32)
            first = e * columns + n * width
            out_ref[:, first : first + width] = summed.astype(bf16)

    for g in range(groups):
        for i, j in sends:
            request_copy(g, i, j).wait_send()
    for g, sub in chunks:
        for i in range(outer - 1):
            target = pick([far[t][i] for t in range(outer)], z)

            @pl.when(is_near(target))
            def _():
                near_copy(g, sub, target).wait_send()

            source = pick([order[t][i] for t in range(outer)], z)

            @pl.when(is_relay(source))
            def _():
                relay_copy(g, sub, source).wait_send()

        sided = chunks.index((g, sub)) < side_chunks
        for j in range(1, inner):
            if sided:
                side_copy(g, sub, j).wait_send()
            for source in range(outer):
                if not sided:
                    across_copy(g, sub, source, j).wait_send()
                    continue

                @pl.when(beside != source)
                def _():
                    across_copy(g, sub, source, j).wait_send()

    swap.wait_send()
    for i, j in sends:
        part_copy(i, j).wait_send()

    @pl.when(target_part != part)
    def _():
        part_copy(outer - 1, 0).wait_send()


def on_device(
    dp,
    mp,
    queries,
    incoming_key,
    incoming_value,
    key_cache,
    cached_values,
    task_key_scale,
    task_value_scale,
    out_weight,
    task_id,
    cached_length,
    task_owner,
    cache_slot,
):
    rows, query_width = queries.shape
    kv_width = incoming_key.shape[1]
    slots, positions, _ = key_cache.shape
    capacity = 2 * rows // dp
    items = dp * capacity
    columns = out_weight.shape[1]
    row_width = query_width + 2 * kv_width + META
    groups = kv_width // HEAD_SIZE
    group_width = GROUP * HEAD_SIZE
    half = slots // 2
    per = half // SUBS
    outer, inner = factors(dp)
    away = pl.BlockSpec(memory_space=pl.ANY)
    small = [
        queries,
        incoming_key,
        incoming_value,
        task_key_scale,
        task_value_scale,
        task_id.reshape(1, -1),
        cached_length.reshape(1, -1),
        cache_slot.reshape(1, -1),
        task_owner.reshape(1, -1),
    ]
    return pl.pallas_call(
        functools.partial(layer_kernel, dp, mp),
        out_shape=pltpu.VMEM((rows, dp * columns // mp), bf16),
        in_specs=[away] * 12,
        out_specs=pl.BlockSpec(memory_space=pltpu.VMEM),
        scratch_shapes=[pltpu.VMEM(a.shape, a.dtype) for a in small]
        + [
            pltpu.VMEM(key_cache.shape, bf16),
            pltpu.VMEM(cached_values.shape, bf16),
            pltpu.VMEM((2, out_weight.shape[0], columns // 2), bf16),
            pltpu.VMEM((items, row_width), f32),
            pltpu.VMEM((items, row_width), f32),
            pltpu.VMEM((dp, 1, META), f32),
            pltpu.VMEM((dp, capacity, row_width), bf16),
            pltpu.VMEM((dp, capacity, row_width), bf16),
            pltpu.VMEM((half, 2 * GROUP, 2 * HEAD_SIZE), f32),
            pltpu.VMEM((3, half, 2 * HEAD_SIZE), f32),
            pltpu.VMEM((slots, kv_width), f32),
            pltpu.VMEM((slots, positions), f32),
            pltpu.VMEM((per, 2 * GROUP, HEAD_SIZE), f32),
            pltpu.VMEM((groups, dp, SUBS, 2 * per, group_width), bf16),
            pltpu.VMEM((dp * rows, dp * slots), bf16),
            pltpu.VMEM((2, dp, rows, columns // 2), f32),
            pltpu.VMEM((dp, rows, columns // 2), bf16),
            pltpu.VMEM((dp, rows, columns // 2), bf16),
            pltpu.VMEM((dp, rows, columns // 2), bf16),
            pltpu.VMEM((dp, rows, columns // 2), bf16),
            pltpu.SemaphoreType.DMA((len(small),)),
            pltpu.SemaphoreType.DMA((4,)),
            pltpu.SemaphoreType.DMA((groups, dp)),
            pltpu.SemaphoreType.DMA((groups, dp)),
            pltpu.SemaphoreType.DMA((outer, groups, SUBS)),
            pltpu.SemaphoreType.DMA((outer, groups, SUBS)),
            pltpu.SemaphoreType.DMA((outer, groups, SUBS)),
            pltpu.SemaphoreType.DMA((outer, inner, groups, SUBS)),
            pltpu.SemaphoreType.DMA((dp, groups, SUBS)),
            pltpu.SemaphoreType.DMA((inner, groups, SUBS)),
            pltpu.SemaphoreType.DMA((2,)),
            pltpu.SemaphoreType.DMA((dp,)),
            pltpu.SemaphoreType.DMA((dp,)),
        ],
        compiler_params=pltpu.CompilerParams(
            collective_id=0, has_side_effects=True, vmem_limit_bytes=60 * 1024 * 1024
        ),
    )(*small, key_cache, cached_values, out_weight)


def solution(mesh):
    placed = (
        P("dp", "mp"),
        P("dp", "mp"),
        P("dp", "mp"),
        P("dp", None, "mp"),
        P("dp", None, "mp"),
        P(None, "mp"),
        P(None, "mp"),
        P("mp", "dp"),
        P("dp"),
        P("dp"),
        P(),
        P("dp"),
    )
    return jax.shard_map(
        functools.partial(on_device, mesh.shape["dp"], mesh.shape["mp"]),
        mesh=mesh,
        in_specs=placed,
        out_specs=P("dp", "mp"),
        check_vma=False,
    )
```

```python
import contextlib
import functools
import math

import jax
import jax.numpy as jnp
from jax import lax
from jax.experimental import pallas as pl
from jax.experimental.pallas import tpu as pltpu
from jax.sharding import PartitionSpec as P

KEY_VALUE_HEADS = 8
HEAD_SIZE = 128
QUERY_HEADS = 64
GROUP = QUERY_HEADS // KEY_VALUE_HEADS
META = 128
FIRST = 16
SUBS = 2
SIDE = 2
SCOPES = False
MESH = pl.DeviceIdType.MESH

masked_score = -1e30
f32 = jnp.float32
bf16 = jnp.bfloat16


def phase(name):
    return jax.named_scope(name) if SCOPES else contextlib.nullcontext()


def iota(shape, dim):
    return lax.broadcasted_iota(jnp.int32, shape, dim)


def to_column(row):
    n = row.shape[1]
    eye = iota((n, n), 0) == iota((n, n), 1)
    return jnp.sum(jnp.where(eye, row, 0.0), axis=1, keepdims=True)


def to_row(column):
    n = column.shape[0]
    eye = iota((n, n), 0) == iota((n, n), 1)
    return jnp.sum(jnp.where(eye, column, 0.0), axis=0, keepdims=True)


def factors(dp):
    inner = 2 ** (int(math.log2(dp)) // 2)
    return dp // inner, inner


def dot(a, b):
    return jnp.dot(a, b, preferred_element_type=f32)


def pick(table, index):
    value = table[0]
    for i in range(1, len(table)):
        value = jnp.where(index == i, table[i], value)
    return value


def far_first(count):
    return [sorted(range(count), key=lambda t: -abs(t - z)) for z in range(count)]


def relays(z, source, count):
    beyond = z + (1 if z > source else -1)
    return abs(z - source) >= 2 and 0 <= beyond < count


def arrival_order(count):
    def rank(z):
        return lambda s: abs(z - s) - (1.5 if relays(z, s, count) else 0.0)

    return [sorted((s for s in range(count) if s != z), key=rank(z)) for z in range(count)]


def layer_kernel(
    dp,
    mp,
    query_hbm,
    new_key_hbm,
    new_value_hbm,
    key_scale_hbm,
    value_scale_hbm,
    task_hbm,
    length_hbm,
    slot_hbm,
    owner_hbm,
    key_hbm,
    value_hbm,
    weight_hbm,
    out_ref,
    query_ref,
    new_key_ref,
    new_value_ref,
    key_scale_ref,
    value_scale_ref,
    task_ref,
    length_ref,
    slot_ref,
    owner_ref,
    keys,
    values,
    weight,
    rows_f32,
    in_f32,
    fact_rows,
    send_rows,
    recv_rows,
    pair_query,
    pair_small,
    value_scale,
    slot_length,
    slot_context,
    context,
    selector,
    total,
    give,
    take,
    send_part,
    recv_part,
    local_sem,
    request_recv,
    along_recv,
    across_recv,
    side_recv,
    last_recv,
):
    me = lax.axis_index("dp")
    part = lax.axis_index("mp")
    rows, query_width = query_ref.shape
    groups = new_key_ref.shape[1] // HEAD_SIZE
    group_width = GROUP * HEAD_SIZE
    segment = group_width + 2 * HEAD_SIZE
    task_total = key_scale_ref.shape[0]
    slots, positions, _ = keys.shape
    capacity = send_rows.shape[1]
    items = dp * capacity
    columns = 2 * weight.shape[2]
    blocks = dp // mp
    half = slots // 2
    per = half // SUBS
    outer, inner = factors(dp)
    z, y = me // inner, lax.rem(me, inner)

    barrier = pltpu.get_barrier_semaphore()
    for k in range(1, dp):
        pl.semaphore_signal(
            barrier, inc=1, device_id=(lax.rem(me + k, dp), part), device_id_type=MESH
        )
    for k in range(1, mp):
        pl.semaphore_signal(
            barrier, inc=1, device_id=(me, lax.rem(part + k, mp)), device_id_type=MESH
        )

    pairs = [
        (task_hbm, task_ref),
        (owner_hbm, owner_ref),
        (length_hbm, length_ref),
        (slot_hbm, slot_ref),
        (key_scale_hbm, key_scale_ref),
        (query_hbm, query_ref),
        (new_key_hbm, new_key_ref),
        (new_value_hbm, new_value_ref),
        (value_scale_hbm, value_scale_ref),
    ]
    inputs = [pltpu.make_async_copy(a, b, local_sem.at[i]) for i, (a, b) in enumerate(pairs)]
    for copy in inputs:
        copy.start()
    parity = lax.rem(part, 2)
    width = weight.shape[2]
    kept_lanes = pl.ds(pl.multiple_of(parity * width, width), width)
    given_lanes = pl.ds(pl.multiple_of((1 - parity) * width, width), width)
    fetches = [
        pltpu.make_async_copy(key_hbm, keys, local_sem.at[0]),
        pltpu.make_async_copy(value_hbm, values, local_sem.at[1]),
        pltpu.make_async_copy(weight_hbm.at[:, given_lanes], weight.at[0], local_sem.at[2]),
        pltpu.make_async_copy(weight_hbm.at[:, kept_lanes], weight.at[1], local_sem.at[2]),
    ]
    pair_query[...] = jnp.zeros_like(pair_query)

    def start_of(g):
        return g * segment + (META if g > 0 else 0)

    def span_of(g):
        return slice(start_of(g), start_of(g) + segment + (META if g == 0 else 0))

    meta = slice(segment, segment + META)

    with phase("inputs"):
        for copy in inputs[:4]:
            copy.wait()
    with phase("pack0"):
        task_column = to_column(task_ref[...].astype(f32))
        length_column = to_column(length_ref[...].astype(f32))
        slot_column = to_column(slot_ref[...].astype(f32))
        picked = task_column == iota((rows, task_total), 1).astype(f32)
        owner_column = jnp.sum(
            jnp.where(picked, owner_ref[...].astype(f32), 0.0), axis=1, keepdims=True
        )
        owner_row = to_row(owner_column)
        earlier = iota((rows, rows), 1) < iota((rows, rows), 0)
        rank = jnp.sum(
            jnp.where(earlier & (owner_column == owner_row), 1.0, 0.0), axis=1, keepdims=True
        )
        position_row = to_row(owner_column * capacity + rank)
        packer = jnp.where(
            position_row == iota((items, rows), 0).astype(f32), 1.0, 0.0
        ).astype(bf16)
        side = jnp.floor(slot_column * (1.0 / half))
        pair = slot_column - side * half
        sub = jnp.floor(pair * (1.0 / per))
        line_column = sub * (2 * per) + side * per + (pair - sub * per)
        lane = iota((rows, META), 1)
        line = iota((rows, META), 0)
        task_high = jnp.floor(task_column * (1.0 / 128.0))
        task_low = task_column - task_high * 128.0
        facts = (
            jnp.where(lane == 0, slot_column + 1.0, 0.0)
            + jnp.where(lane == 1, length_column, 0.0)
            + jnp.where(lane == 2, task_high, 0.0)
            + jnp.where(lane == 3, task_low, 0.0)
        )
        shared = jnp.sum(
            jnp.where(lane == FIRST + line, owner_column, 0.0)
            + jnp.where(lane == FIRST + rows + line, line_column, 0.0),
            axis=0,
            keepdims=True,
        )
        rows_f32[:, meta] = dot(packer, facts.astype(bf16)) + shared
        for copy in inputs[4:]:
            copy.wait()
        for fetch in fetches:
            fetch.start()
        key_factor = dot(jnp.where(picked, 1.0, 0.0).astype(bf16), key_scale_ref[...])

    def pack(g):
        own = slice(g * HEAD_SIZE, (g + 1) * HEAD_SIZE)
        at = start_of(g)
        for h in range(GROUP):
            lanes = slice((g * GROUP + h) * HEAD_SIZE, (g * GROUP + h + 1) * HEAD_SIZE)
            scaled = (query_ref[:, lanes].astype(f32) * key_factor[:, own]).astype(bf16)
            rows_f32[:, at + h * HEAD_SIZE : at + (h + 1) * HEAD_SIZE] = dot(packer, scaled)
        first = key_at(g)
        rows_f32[:, first : first + HEAD_SIZE] = dot(packer, new_key_ref[:, own])
        rows_f32[:, first + HEAD_SIZE : first + 2 * HEAD_SIZE] = dot(packer, new_value_ref[:, own])
        for d in range(dp):
            send_rows[d, :, span_of(g)] = rows_f32[
                d * capacity : (d + 1) * capacity, span_of(g)
            ].astype(bf16)

    def key_at(g):
        return start_of(g) + group_width

    far = far_first(outer)
    sends = [(i, j) for i in range(outer) for j in range(inner - 1, -1, -1)][:-1]

    def request_copy(g, i, j):
        target = pick([far[t][i] for t in range(outer)], z) * inner + lax.rem(y + j, inner)
        return pltpu.make_async_remote_copy(
            src_ref=send_rows.at[target, :, span_of(g)],
            dst_ref=recv_rows.at[me, :, span_of(g)],
            send_sem=local_sem.at[3],
            recv_sem=request_recv.at[g],
            device_id=(target, part),
            device_id_type=MESH,
        )

    def requests_done(g):
        slab = recv_rows.at[pl.ds(0, dp - 1), :, span_of(g)]
        return pltpu.make_async_copy(slab, slab, request_recv.at[g])

    with phase("pack1"):
        pack(0)
    with phase("barrier"):
        pl.semaphore_wait(barrier, dp + mp - 2)
    for g in range(groups):
        if g > 0:
            with phase("pack2"):
                pack(g)
        for i, j in sends:
            request_copy(g, i, j).start()
    recv_rows[me] = send_rows[me]

    inv_root = 1.0 / math.sqrt(HEAD_SIZE)
    key_line = iota((2 * GROUP, positions), 1).astype(f32)
    low_line = iota((2 * GROUP, positions), 0) < GROUP

    def attend(g, sub):
        own = slice(g * HEAD_SIZE, (g + 1) * HEAD_SIZE)
        picks = [sub * per + i for i in range(per)]

        def both(ref, p):
            return jnp.concatenate([ref[p, :, own], ref[p + half, :, own]], axis=1)

        scores, owns, weights, own_weights, tops, shows, sees = [], [], [], [], [], [], []
        for p in picks:
            scores.append(
                lax.dot_general(
                    pair_query[p].astype(bf16),
                    both(keys, p),
                    (((1,), (1,)), ((), ())),
                    preferred_element_type=f32,
                )
                * inv_root
            )
        for p in picks:
            owns.append(
                jnp.sum(pair_query[p] * pair_small[0, p : p + 1, :], axis=1, keepdims=True)
                * inv_root
            )
        for i, p in enumerate(picks):
            length = jnp.where(
                low_line, slot_length[p : p + 1, :], slot_length[p + half : p + half + 1, :]
            )
            sees.append(key_line < length)
            shows.append(jnp.where(sees[i], scores[i], masked_score))
            tops.append(jnp.maximum(jnp.max(shows[i], axis=1, keepdims=True), owns[i]))
        for i in range(per):
            weights.append(jnp.where(sees[i], jnp.exp(shows[i] - tops[i]), 0.0))
            own_weights.append(jnp.exp(owns[i] - tops[i]))
        blends = [dot(weights[i].astype(bf16), both(values, p)) for i, p in enumerate(picks)]
        for i, p in enumerate(picks):
            weight_sum = jnp.sum(weights[i], axis=1, keepdims=True) + own_weights[i]
            one = slice(p, p + 1)
            blended = blends[i] + own_weights[i].astype(bf16).astype(f32) * pair_small[1, one, :]
            attended = (blended / weight_sum).astype(bf16).astype(f32) * pair_small[2, one, :]
            slot_context[i, :GROUP, :] = attended[:GROUP, :HEAD_SIZE]
            slot_context[i, GROUP:, :] = attended[GROUP:, HEAD_SIZE:]
        for h in range(GROUP):
            context[g, me, sub, :, h * HEAD_SIZE : (h + 1) * HEAD_SIZE] = jnp.concatenate(
                [slot_context[:, h, :], slot_context[:, GROUP + h, :]], axis=0
            ).astype(bf16)

    def near_copy(g, sub, target):
        return pltpu.make_async_remote_copy(
            src_ref=context.at[g, me, sub],
            dst_ref=context.at[g, me, sub],
            send_sem=local_sem.at[4],
            recv_sem=along_recv.at[z - jnp.where(z > target, 1, 0), g, sub],
            device_id=(target * inner + y, part),
            device_id_type=MESH,
        )

    def is_near(target):
        return (target != z) & (target - z < 3) & (z - target < 3)

    def along_arrival(g, sub, source):
        at = source * inner + y
        return pltpu.make_async_remote_copy(
            src_ref=context.at[g, at, sub],
            dst_ref=context.at[g, at, sub],
            send_sem=local_sem.at[4],
            recv_sem=along_recv.at[source - jnp.where(source > z, 1, 0), g, sub],
            device_id=(at, part),
            device_id_type=MESH,
        )

    def relay_copy(g, sub, source):
        at = source * inner + y
        beyond = z + jnp.where(z > source, 1, -1)
        return pltpu.make_async_remote_copy(
            src_ref=context.at[g, at, sub],
            dst_ref=context.at[g, at, sub],
            send_sem=local_sem.at[4],
            recv_sem=along_recv.at[source - jnp.where(source > beyond, 1, 0), g, sub],
            device_id=(beyond * inner + y, part),
            device_id_type=MESH,
        )

    def is_relay(source):
        up = (z - source >= 2) & (z < outer - 1)
        down = (source - z >= 2) & (z > 0)
        return up | down

    def across_copy(g, sub, source, j):
        at = source * inner + y
        return pltpu.make_async_remote_copy(
            src_ref=context.at[g, at, sub],
            dst_ref=context.at[g, at, sub],
            send_sem=local_sem.at[5],
            recv_sem=across_recv.at[g],
            device_id=(z * inner + lax.rem(y + j, inner), part),
            device_id_type=MESH,
        )

    def side_first(g, sub, j):
        at = z * inner + lax.rem(y + j, inner)
        return pltpu.make_async_remote_copy(
            src_ref=context.at[g, me, sub],
            dst_ref=context.at[g, me, sub],
            send_sem=local_sem.at[5],
            recv_sem=side_recv.at[g, sub, inner - j - 1],
            device_id=(at, part),
            device_id_type=MESH,
        )

    def side_arrival(g, sub, j):
        at = z * inner + lax.rem(y + j, inner)
        return pltpu.make_async_remote_copy(
            src_ref=context.at[g, at, sub],
            dst_ref=context.at[g, at, sub],
            send_sem=local_sem.at[5],
            recv_sem=side_recv.at[g, sub, j - 1],
            device_id=(at, part),
            device_id_type=MESH,
        )

    def across_done(g):
        count = (outer - 1 if is_sided(g) else outer) * (inner - 1)
        slab = context.at[g, pl.ds(0, count)]
        return pltpu.make_async_copy(slab, slab, across_recv.at[g])

    def is_sided(g):
        return g < SIDE * groups // 4

    chunks = [(g, sub) for g in range(groups) for sub in range(SUBS)]
    for g in range(groups):
        with phase("requests"):
            requests_done(g).wait()
        with phase("place"):
            for s in range(dp):
                in_f32[s * capacity : (s + 1) * capacity, span_of(g)] = recv_rows[
                    s, :, span_of(g)
                ].astype(f32)
            if g == 0:
                facts_in = in_f32[:, meta]
                for s in range(dp):
                    fact_rows[s] = in_f32[s * capacity : s * capacity + 1, meta]
                placing_row = to_row(facts_in[:, 0:1])
                placer = jnp.where(
                    placing_row == iota((slots, items), 0).astype(f32) + 1.0, 1.0, 0.0
                ).astype(bf16)
                slot_facts = dot(placer, facts_in.astype(bf16))
                slot_task = slot_facts[:, 2:3] * 128.0 + slot_facts[:, 3:4]
                value_scale[...] = dot(
                    jnp.where(slot_task == iota((slots, task_total), 1).astype(f32), 1.0, 0.0).astype(bf16),
                    value_scale_ref[...],
                )
                slot_length[...] = jnp.broadcast_to(slot_facts[:, 1:2], (slots, positions))
            at = start_of(g)
            for h in range(GROUP):
                placed = dot(
                    placer, in_f32[:, at + h * HEAD_SIZE : at + (h + 1) * HEAD_SIZE].astype(bf16)
                )
                pair_query[:, h, :HEAD_SIZE] = placed[:half]
                pair_query[:, GROUP + h, HEAD_SIZE:] = placed[half:]
            for i in range(2):
                first = key_at(g) + i * HEAD_SIZE
                small = dot(placer, in_f32[:, first : first + HEAD_SIZE].astype(bf16))
                pair_small[i, :, :HEAD_SIZE] = small[:half]
                pair_small[i, :, HEAD_SIZE:] = small[half:]
            own = slice(g * HEAD_SIZE, (g + 1) * HEAD_SIZE)
            pair_small[2, :, :HEAD_SIZE] = value_scale[:half, own]
            pair_small[2, :, HEAD_SIZE:] = value_scale[half:, own]
        if g == 0:
            with phase("fetch"):
                fetches[0].wait()
                fetches[1].wait()
        for sub in range(SUBS):
            with phase("attend"):
                attend(g, sub)
            for j in range(1, inner):
                (side_first(g, sub, j) if is_sided(g) else across_copy(g, sub, z, j)).start()
            for i in range(outer - 1):
                target = pick([far[t][i] for t in range(outer)], z)

                @pl.when(is_near(target))
                def _():
                    near_copy(g, sub, target).start()

    with phase("selector"):
        lane_r = iota((rows, META), 1)
        line_r = iota((rows, META), 0)
        for i in range(dp):
            fact_row = fact_rows[i]
            owner_in = jnp.sum(
                jnp.where(lane_r == FIRST + line_r, fact_row, 0.0), axis=1, keepdims=True
            )
            line_in = jnp.sum(
                jnp.where(lane_r == FIRST + rows + line_r, fact_row, 0.0), axis=1, keepdims=True
            )
            selector[i * rows : (i + 1) * rows, :] = jnp.where(
                owner_in * slots + line_in == iota((rows, dp * slots), 1).astype(f32), 1.0, 0.0
            ).astype(bf16)

    beside = z + 1 - 2 * lax.rem(z, 2)

    def side_copy(g, sub, j):
        at = z * inner + lax.rem(y + j, inner)
        return pltpu.make_async_remote_copy(
            src_ref=context.at[g, at, sub],
            dst_ref=context.at[g, at, sub],
            send_sem=local_sem.at[5],
            recv_sem=across_recv.at[g],
            device_id=(beside * inner + y, part),
            device_id_type=MESH,
        )

    order = arrival_order(outer)
    late = outer - 2
    events = sorted(
        [(c + (1.5 if r >= late else 0.0), r, c) for c in range(len(chunks)) for r in range(outer - 1)]
        + [(c - 0.5, -1, c) for c, (g, _) in enumerate(chunks) if is_sided(g)]
    )
    with phase("forward"):
        for _, r, c in events:
            g, sub = chunks[c]
            if r < 0:
                for j in range(1, inner):
                    side_arrival(g, sub, j).wait_recv()
                    side_copy(g, sub, j).start()
                continue
            source = pick([order[t][r] for t in range(outer)], z)
            along_arrival(g, sub, source).wait_recv()

            @pl.when(is_relay(source))
            def _():
                relay_copy(g, sub, source).start()

            if is_sided(g):

                @pl.when(source != beside)
                def _():
                    for j in range(1, inner):
                        across_copy(g, sub, source, j).start()

            else:
                for j in range(1, inner):
                    across_copy(g, sub, source, j).start()

    pltpu.make_async_copy(weight, weight, local_sem.at[2]).wait()

    def arrange(g):
        blocks_of = context[g].reshape(dp * slots, group_width)
        return dot(selector[...], blocks_of).astype(bf16)

    def product(arranged, g, n):
        found = dot(arranged, weight[n, g * group_width : (g + 1) * group_width, :])
        return found.reshape(dp, rows, width)

    for g in range(groups - 1):
        with phase("across"):
            across_done(g).wait()
        with phase("product"):
            arranged = arrange(g)
            for n in range(2):
                found = product(arranged, g, n)
                total[n] = found if g == 0 else total[n] + found
    with phase("across"):
        across_done(groups - 1).wait()

    partner = part + 1 - 2 * parity
    swap = pltpu.make_async_remote_copy(
        src_ref=give,
        dst_ref=take,
        send_sem=local_sem.at[6],
        recv_sem=last_recv.at[0],
        device_id=(me, partner),
        device_id_type=MESH,
    )
    with phase("product"):
        arranged = arrange(groups - 1)
        given = product(arranged, groups - 1, 0)
        give[...] = (given if groups == 1 else given + total[0]).astype(bf16)
    swap.start()
    with phase("product"):
        kept = product(arranged, groups - 1, 1)
        total[1] = kept if groups == 1 else kept + total[1]
    with phase("swap"):
        swap.wait_recv()

    target_part = me // blocks
    place = lax.rem(me, blocks) * mp + part

    def part_target(i, j):
        return pick([far[t][i] for t in range(outer)], z) * inner + lax.rem(y + j, inner)

    def part_copy(i, j):
        target = part_target(i, j)
        return pltpu.make_async_remote_copy(
            src_ref=send_part.at[target],
            dst_ref=recv_part.at[place],
            send_sem=local_sem.at[7],
            recv_sem=last_recv.at[1],
            device_id=(target, target_part),
            device_id_type=MESH,
        )
    def parts_wait(buffer, count, semaphore):
        slab = buffer.at[pl.ds(0, count)]
        pltpu.make_async_copy(slab, slab, semaphore).wait()

    with phase("parts"):
        for i, j in sends + [(outer - 1, 0)]:
            target = part_target(i, j)
            send_part[target] = (total[1, target] + take[target].astype(f32)).astype(bf16)
            if (i, j) in sends:
                part_copy(i, j).start()

        @pl.when(target_part != part)
        def _():
            part_copy(outer - 1, 0).start()

        @pl.when(target_part == part)
        def _():
            recv_part[place] = send_part[me]

        @pl.when(target_part != part)
        def _():
            parts_wait(recv_part, dp, last_recv.at[1])

        @pl.when(target_part == part)
        def _():
            parts_wait(recv_part, dp - 1, last_recv.at[1])

    with phase("sum"):
        for e in range(blocks):
            for n in range(2):
                summed = recv_part[e * mp + n].astype(f32)
                for j in range(n + 2, mp, 2):
                    summed = summed + recv_part[e * mp + j].astype(f32)
                first = e * columns + n * width
                out_ref[:, first : first + width] = summed.astype(bf16)

    with phase("drain"):
        slab = send_rows.at[pl.ds(0, dp - 1)]
        pltpu.make_async_copy(slab, slab, local_sem.at[3]).wait()
        for t in range(outer):
            near = min(2, t) + min(2, outer - 1 - t)
            relayed = sum(relays(t, s, outer) for s in range(outer))

            @pl.when(z == t)
            def _():
                slab = context.at[:, pl.ds(0, near + relayed)]
                pltpu.make_async_copy(slab, slab, local_sem.at[4]).wait()

        slab = context.at[:, pl.ds(0, outer * (inner - 1))]
        pltpu.make_async_copy(slab, slab, local_sem.at[5]).wait()
        swap.wait_send()

        @pl.when(target_part != part)
        def _():
            parts_wait(send_part, dp, local_sem.at[7])

        @pl.when(target_part == part)
        def _():
            parts_wait(send_part, dp - 1, local_sem.at[7])


def on_device(
    dp,
    mp,
    queries,
    incoming_key,
    incoming_value,
    key_cache,
    cached_values,
    task_key_scale,
    task_value_scale,
    out_weight,
    task_id,
    cached_length,
    task_owner,
    cache_slot,
):
    rows, query_width = queries.shape
    kv_width = incoming_key.shape[1]
    slots, positions, _ = key_cache.shape
    capacity = 2 * rows // dp
    items = dp * capacity
    columns = out_weight.shape[1]
    row_width = query_width + 2 * kv_width + META
    groups = kv_width // HEAD_SIZE
    group_width = GROUP * HEAD_SIZE
    half = slots // 2
    per = half // SUBS
    outer, inner = factors(dp)
    away = pl.BlockSpec(memory_space=pl.ANY)
    small = [
        queries,
        incoming_key,
        incoming_value,
        task_key_scale,
        task_value_scale,
        task_id.reshape(1, -1),
        cached_length.reshape(1, -1),
        cache_slot.reshape(1, -1),
        task_owner.reshape(1, -1),
    ]
    return pl.pallas_call(
        functools.partial(layer_kernel, dp, mp),
        out_shape=pltpu.VMEM((rows, dp * columns // mp), bf16),
        in_specs=[away] * 12,
        out_specs=pl.BlockSpec(memory_space=pltpu.VMEM),
        scratch_shapes=[pltpu.VMEM(a.shape, a.dtype) for a in small]
        + [
            pltpu.VMEM(key_cache.shape, bf16),
            pltpu.VMEM(cached_values.shape, bf16),
            pltpu.VMEM((2, out_weight.shape[0], columns // 2), bf16),
            pltpu.VMEM((items, row_width), f32),
            pltpu.VMEM((items, row_width), f32),
            pltpu.VMEM((dp, 1, META), f32),
            pltpu.VMEM((dp, capacity, row_width), bf16),
            pltpu.VMEM((dp, capacity, row_width), bf16),
            pltpu.VMEM((half, 2 * GROUP, 2 * HEAD_SIZE), f32),
            pltpu.VMEM((3, half, 2 * HEAD_SIZE), f32),
            pltpu.VMEM((slots, kv_width), f32),
            pltpu.VMEM((slots, positions), f32),
            pltpu.VMEM((per, 2 * GROUP, HEAD_SIZE), f32),
            pltpu.VMEM((groups, dp, SUBS, 2 * per, group_width), bf16),
            pltpu.VMEM((dp * rows, dp * slots), bf16),
            pltpu.VMEM((2, dp, rows, columns // 2), f32),
            pltpu.VMEM((dp, rows, columns // 2), bf16),
            pltpu.VMEM((dp, rows, columns // 2), bf16),
            pltpu.VMEM((dp, rows, columns // 2), bf16),
            pltpu.VMEM((dp, rows, columns // 2), bf16),
            pltpu.SemaphoreType.DMA((len(small),)),
            pltpu.SemaphoreType.DMA((groups,)),
            pltpu.SemaphoreType.DMA((outer - 1, groups, SUBS)),
            pltpu.SemaphoreType.DMA((groups,)),
            pltpu.SemaphoreType.DMA((max(groups // 2, 1), SUBS, inner - 1)),
            pltpu.SemaphoreType.DMA((2,)),
        ],
        compiler_params=pltpu.CompilerParams(
            collective_id=0, has_side_effects=True, vmem_limit_bytes=60 * 1024 * 1024
        ),
    )(*small, key_cache, cached_values, out_weight)


def solution(mesh):
    placed = (
        P("dp", "mp"),
        P("dp", "mp"),
        P("dp", "mp"),
        P("dp", None, "mp"),
        P("dp", None, "mp"),
        P(None, "mp"),
        P(None, "mp"),
        P("mp", "dp"),
        P("dp"),
        P("dp"),
        P(),
        P("dp"),
    )
    return jax.shard_map(
        functools.partial(on_device, mesh.shape["dp"], mesh.shape["mp"]),
        mesh=mesh,
        in_specs=placed,
        out_specs=P("dp", "mp"),
        check_vma=False,
    )
```

```python
import contextlib
import functools
import math

import jax
import jax.numpy as jnp
from jax import lax
from jax.experimental import pallas as pl
from jax.experimental.pallas import tpu as pltpu
from jax.sharding import PartitionSpec as P

KEY_VALUE_HEADS = 8
HEAD_SIZE = 128
QUERY_HEADS = 64
GROUP = QUERY_HEADS // KEY_VALUE_HEADS
META = 128
FIRST = 16
SUBS = 2
SIDE = 2
END_SIDE = 2.3
END_LAG = (0.0, 3.5, 3.6)
MID_LAG = (0.0, 0.1, 0.2)
SCOPES = False
MESH = pl.DeviceIdType.MESH

masked_score = -1e30
f32 = jnp.float32
bf16 = jnp.bfloat16


def phase(name):
    return jax.named_scope(name) if SCOPES else contextlib.nullcontext()


def iota(shape, dim):
    return lax.broadcasted_iota(jnp.int32, shape, dim)


def to_column(row):
    n = row.shape[1]
    eye = iota((n, n), 0) == iota((n, n), 1)
    return jnp.sum(jnp.where(eye, row, 0.0), axis=1, keepdims=True)


def to_row(column):
    n = column.shape[0]
    eye = iota((n, n), 0) == iota((n, n), 1)
    return jnp.sum(jnp.where(eye, column, 0.0), axis=0, keepdims=True)


def factors(dp):
    inner = 2 ** (int(math.log2(dp)) // 2)
    return dp // inner, inner


def dot(a, b):
    return jnp.dot(a, b, preferred_element_type=f32)


def pick(table, index):
    value = table[0]
    for i in range(1, len(table)):
        value = jnp.where(index == i, table[i], value)
    return value


def far_first(count):
    return [sorted(range(count), key=lambda t: -abs(t - z)) for z in range(count)]


def is_near(source, target, count):
    apart = abs(source - target)
    return apart == 1 or (apart == 2 and 0 < target < count - 1)


def relays(z, source, count):
    beyond = z + (1 if z > source else -1)
    return z != source and 0 <= beyond < count and not is_near(source, beyond, count)


def arrival_order(count):
    def rank(z):
        return lambda s: abs(z - s) - (1.5 if relays(z, s, count) else 0.0)

    return [sorted((s for s in range(count) if s != z), key=rank(z)) for z in range(count)]


def layer_kernel(
    dp,
    mp,
    query_hbm,
    new_key_hbm,
    new_value_hbm,
    key_scale_hbm,
    value_scale_hbm,
    task_hbm,
    length_hbm,
    slot_hbm,
    owner_hbm,
    key_hbm,
    value_hbm,
    weight_hbm,
    out_ref,
    query_ref,
    new_key_ref,
    new_value_ref,
    key_scale_ref,
    value_scale_ref,
    task_ref,
    length_ref,
    slot_ref,
    owner_ref,
    keys,
    values,
    weight,
    rows_f32,
    in_f32,
    fact_rows,
    send_rows,
    recv_rows,
    pair_query,
    pair_small,
    value_scale,
    slot_length,
    slot_context,
    context,
    selector,
    total,
    give,
    take,
    send_part,
    recv_part,
    local_sem,
    request_recv,
    along_recv,
    across_recv,
    side_recv,
    last_recv,
):
    me = lax.axis_index("dp")
    part = lax.axis_index("mp")
    rows, query_width = query_ref.shape
    groups = new_key_ref.shape[1] // HEAD_SIZE
    group_width = GROUP * HEAD_SIZE
    segment = group_width + 2 * HEAD_SIZE
    task_total = key_scale_ref.shape[0]
    slots, positions, _ = keys.shape
    capacity = send_rows.shape[1]
    items = dp * capacity
    columns = 2 * weight.shape[2]
    blocks = dp // mp
    half = slots // 2
    per = half // SUBS
    outer, inner = factors(dp)
    z, y = me // inner, lax.rem(me, inner)

    barrier = pltpu.get_barrier_semaphore()
    for k in range(1, dp):
        pl.semaphore_signal(
            barrier, inc=1, device_id=(lax.rem(me + k, dp), part), device_id_type=MESH
        )
    for k in range(1, mp):
        pl.semaphore_signal(
            barrier, inc=1, device_id=(me, lax.rem(part + k, mp)), device_id_type=MESH
        )

    pairs = [
        (task_hbm, task_ref),
        (owner_hbm, owner_ref),
        (length_hbm, length_ref),
        (slot_hbm, slot_ref),
        (key_scale_hbm, key_scale_ref),
        (query_hbm, query_ref),
        (new_key_hbm, new_key_ref),
        (new_value_hbm, new_value_ref),
        (value_scale_hbm, value_scale_ref),
    ]
    inputs = [pltpu.make_async_copy(a, b, local_sem.at[i]) for i, (a, b) in enumerate(pairs)]
    for copy in inputs:
        copy.start()
    parity = lax.rem(part, 2)
    width = weight.shape[2]
    kept_lanes = pl.ds(pl.multiple_of(parity * width, width), width)
    given_lanes = pl.ds(pl.multiple_of((1 - parity) * width, width), width)
    fetches = [
        pltpu.make_async_copy(key_hbm, keys, local_sem.at[0]),
        pltpu.make_async_copy(value_hbm, values, local_sem.at[1]),
        pltpu.make_async_copy(weight_hbm.at[:, given_lanes], weight.at[0], local_sem.at[2]),
        pltpu.make_async_copy(weight_hbm.at[:, kept_lanes], weight.at[1], local_sem.at[2]),
    ]
    pair_query[...] = jnp.zeros_like(pair_query)

    def start_of(g):
        return g * segment + (META if g > 0 else 0)

    def span_of(g):
        return slice(start_of(g), start_of(g) + segment + (META if g == 0 else 0))

    meta = slice(segment, segment + META)

    with phase("inputs"):
        for copy in inputs[:4]:
            copy.wait()
    with phase("pack0"):
        task_column = to_column(task_ref[...].astype(f32))
        length_column = to_column(length_ref[...].astype(f32))
        slot_column = to_column(slot_ref[...].astype(f32))
        picked = task_column == iota((rows, task_total), 1).astype(f32)
        owner_column = jnp.sum(
            jnp.where(picked, owner_ref[...].astype(f32), 0.0), axis=1, keepdims=True
        )
        owner_row = to_row(owner_column)
        earlier = iota((rows, rows), 1) < iota((rows, rows), 0)
        rank = jnp.sum(
            jnp.where(earlier & (owner_column == owner_row), 1.0, 0.0), axis=1, keepdims=True
        )
        position_row = to_row(owner_column * capacity + rank)
        packer = jnp.where(
            position_row == iota((items, rows), 0).astype(f32), 1.0, 0.0
        ).astype(bf16)
        side = jnp.floor(slot_column * (1.0 / half))
        pair = slot_column - side * half
        sub = jnp.floor(pair * (1.0 / per))
        line_column = sub * (2 * per) + side * per + (pair - sub * per)
        lane = iota((rows, META), 1)
        line = iota((rows, META), 0)
        task_high = jnp.floor(task_column * (1.0 / 128.0))
        task_low = task_column - task_high * 128.0
        facts = (
            jnp.where(lane == 0, slot_column + 1.0, 0.0)
            + jnp.where(lane == 1, length_column, 0.0)
            + jnp.where(lane == 2, task_high, 0.0)
            + jnp.where(lane == 3, task_low, 0.0)
        )
        shared = jnp.sum(
            jnp.where(lane == FIRST + line, owner_column, 0.0)
            + jnp.where(lane == FIRST + rows + line, line_column, 0.0),
            axis=0,
            keepdims=True,
        )
        rows_f32[:, meta] = dot(packer, facts.astype(bf16)) + shared
        for copy in inputs[4:]:
            copy.wait()
        for fetch in fetches:
            fetch.start()
        key_factor = dot(jnp.where(picked, 1.0, 0.0).astype(bf16), key_scale_ref[...])

    def pack(g):
        own = slice(g * HEAD_SIZE, (g + 1) * HEAD_SIZE)
        at = start_of(g)
        for h in range(GROUP):
            lanes = slice((g * GROUP + h) * HEAD_SIZE, (g * GROUP + h + 1) * HEAD_SIZE)
            scaled = (query_ref[:, lanes].astype(f32) * key_factor[:, own]).astype(bf16)
            rows_f32[:, at + h * HEAD_SIZE : at + (h + 1) * HEAD_SIZE] = dot(packer, scaled)
        first = key_at(g)
        rows_f32[:, first : first + HEAD_SIZE] = dot(packer, new_key_ref[:, own])
        rows_f32[:, first + HEAD_SIZE : first + 2 * HEAD_SIZE] = dot(packer, new_value_ref[:, own])
        for d in range(dp):
            send_rows[d, :, span_of(g)] = rows_f32[
                d * capacity : (d + 1) * capacity, span_of(g)
            ].astype(bf16)

    def key_at(g):
        return start_of(g) + group_width

    far = far_first(outer)
    sends = [(i, j) for i in range(outer) for j in range(inner - 1, -1, -1)][:-1]

    def request_copy(g, i, j):
        target = pick([far[t][i] for t in range(outer)], z) * inner + lax.rem(y + j, inner)
        return pltpu.make_async_remote_copy(
            src_ref=send_rows.at[target, :, span_of(g)],
            dst_ref=recv_rows.at[me, :, span_of(g)],
            send_sem=local_sem.at[3],
            recv_sem=request_recv.at[g],
            device_id=(target, part),
            device_id_type=MESH,
        )

    def requests_done(g):
        slab = recv_rows.at[pl.ds(0, dp - 1), :, span_of(g)]
        return pltpu.make_async_copy(slab, slab, request_recv.at[g])

    with phase("pack1"):
        pack(0)
    with phase("barrier"):
        pl.semaphore_wait(barrier, dp + mp - 2)
    for g in range(groups):
        if g > 0:
            with phase("pack2"):
                pack(g)
        for i, j in sends:
            request_copy(g, i, j).start()
    recv_rows[me] = send_rows[me]

    inv_root = 1.0 / math.sqrt(HEAD_SIZE)
    key_line = iota((2 * GROUP, positions), 1).astype(f32)
    low_line = iota((2 * GROUP, positions), 0) < GROUP

    def attend(g, sub):
        own = slice(g * HEAD_SIZE, (g + 1) * HEAD_SIZE)
        picks = [sub * per + i for i in range(per)]

        def both(ref, p):
            return jnp.concatenate([ref[p, :, own], ref[p + half, :, own]], axis=1)

        scores, owns, weights, own_weights, tops, shows, sees = [], [], [], [], [], [], []
        for p in picks:
            scores.append(
                lax.dot_general(
                    pair_query[p].astype(bf16),
                    both(keys, p),
                    (((1,), (1,)), ((), ())),
                    preferred_element_type=f32,
                )
                * inv_root
            )
        for p in picks:
            owns.append(
                jnp.sum(pair_query[p] * pair_small[0, p : p + 1, :], axis=1, keepdims=True)
                * inv_root
            )
        for i, p in enumerate(picks):
            length = jnp.where(
                low_line, slot_length[p : p + 1, :], slot_length[p + half : p + half + 1, :]
            )
            sees.append(key_line < length)
            shows.append(jnp.where(sees[i], scores[i], masked_score))
            tops.append(jnp.maximum(jnp.max(shows[i], axis=1, keepdims=True), owns[i]))
        for i in range(per):
            weights.append(jnp.where(sees[i], jnp.exp(shows[i] - tops[i]), 0.0))
            own_weights.append(jnp.exp(owns[i] - tops[i]))
        blends = [dot(weights[i].astype(bf16), both(values, p)) for i, p in enumerate(picks)]
        for i, p in enumerate(picks):
            weight_sum = jnp.sum(weights[i], axis=1, keepdims=True) + own_weights[i]
            one = slice(p, p + 1)
            blended = blends[i] + own_weights[i].astype(bf16).astype(f32) * pair_small[1, one, :]
            attended = (blended / weight_sum).astype(bf16).astype(f32) * pair_small[2, one, :]
            slot_context[i, :GROUP, :] = attended[:GROUP, :HEAD_SIZE]
            slot_context[i, GROUP:, :] = attended[GROUP:, HEAD_SIZE:]
        for h in range(GROUP):
            context[g, me, sub, :, h * HEAD_SIZE : (h + 1) * HEAD_SIZE] = jnp.concatenate(
                [slot_context[:, h, :], slot_context[:, GROUP + h, :]], axis=0
            ).astype(bf16)

    def near_copy(g, sub, target):
        return pltpu.make_async_remote_copy(
            src_ref=context.at[g, me, sub],
            dst_ref=context.at[g, me, sub],
            send_sem=local_sem.at[4],
            recv_sem=along_recv.at[z - jnp.where(z > target, 1, 0), g, sub],
            device_id=(target * inner + y, part),
            device_id_type=MESH,
        )

    def along_arrival(g, sub, source):
        at = source * inner + y
        return pltpu.make_async_remote_copy(
            src_ref=context.at[g, at, sub],
            dst_ref=context.at[g, at, sub],
            send_sem=local_sem.at[4],
            recv_sem=along_recv.at[source - jnp.where(source > z, 1, 0), g, sub],
            device_id=(at, part),
            device_id_type=MESH,
        )

    def relay_copy(g, sub, source):
        at = source * inner + y
        beyond = z + jnp.where(z > source, 1, -1)
        return pltpu.make_async_remote_copy(
            src_ref=context.at[g, at, sub],
            dst_ref=context.at[g, at, sub],
            send_sem=local_sem.at[4],
            recv_sem=along_recv.at[source - jnp.where(source > beyond, 1, 0), g, sub],
            device_id=(beyond * inner + y, part),
            device_id_type=MESH,
        )

    def across_copy(g, sub, source, j):
        at = source * inner + y
        return pltpu.make_async_remote_copy(
            src_ref=context.at[g, at, sub],
            dst_ref=context.at[g, at, sub],
            send_sem=local_sem.at[5],
            recv_sem=across_recv.at[g],
            device_id=(z * inner + lax.rem(y + j, inner), part),
            device_id_type=MESH,
        )

    def side_first(g, sub, j):
        at = z * inner + lax.rem(y + j, inner)
        return pltpu.make_async_remote_copy(
            src_ref=context.at[g, me, sub],
            dst_ref=context.at[g, me, sub],
            send_sem=local_sem.at[5],
            recv_sem=side_recv.at[g, sub, inner - j - 1],
            device_id=(at, part),
            device_id_type=MESH,
        )

    def side_arrival(g, sub, j):
        at = z * inner + lax.rem(y + j, inner)
        return pltpu.make_async_remote_copy(
            src_ref=context.at[g, at, sub],
            dst_ref=context.at[g, at, sub],
            send_sem=local_sem.at[5],
            recv_sem=side_recv.at[g, sub, j - 1],
            device_id=(at, part),
            device_id_type=MESH,
        )

    def across_done(g):
        def wait(sources):
            slab = context.at[g, pl.ds(0, sources * (inner - 1))]
            pltpu.make_async_copy(slab, slab, across_recv.at[g]).wait()

        if not is_sided(g):
            wait(outer)
            return

        @pl.when(at_end)
        def _():
            wait(outer - 1)

        @pl.when(jnp.logical_not(at_end))
        def _():
            wait(outer)

    def is_sided(g):
        return g >= groups - SIDE * groups // 4

    at_end = (z == 0) | (z == outer - 1)
    beside = z + 1 - 2 * lax.rem(z, 2)
    fed = (z == 1) | (z == outer - 2)
    chunks = [(g, sub) for g in range(groups) for sub in range(SUBS)]
    for g in range(groups):
        with phase("requests"):
            requests_done(g).wait()
        with phase("place"):
            for s in range(dp):
                in_f32[s * capacity : (s + 1) * capacity, span_of(g)] = recv_rows[
                    s, :, span_of(g)
                ].astype(f32)
            if g == 0:
                facts_in = in_f32[:, meta]
                for s in range(dp):
                    fact_rows[s] = in_f32[s * capacity : s * capacity + 1, meta]
                placing_row = to_row(facts_in[:, 0:1])
                placer = jnp.where(
                    placing_row == iota((slots, items), 0).astype(f32) + 1.0, 1.0, 0.0
                ).astype(bf16)
                slot_facts = dot(placer, facts_in.astype(bf16))
                slot_task = slot_facts[:, 2:3] * 128.0 + slot_facts[:, 3:4]
                value_scale[...] = dot(
                    jnp.where(slot_task == iota((slots, task_total), 1).astype(f32), 1.0, 0.0).astype(bf16),
                    value_scale_ref[...],
                )
                slot_length[...] = jnp.broadcast_to(slot_facts[:, 1:2], (slots, positions))
            at = start_of(g)
            for h in range(GROUP):
                placed = dot(
                    placer, in_f32[:, at + h * HEAD_SIZE : at + (h + 1) * HEAD_SIZE].astype(bf16)
                )
                pair_query[:, h, :HEAD_SIZE] = placed[:half]
                pair_query[:, GROUP + h, HEAD_SIZE:] = placed[half:]
            for i in range(2):
                first = key_at(g) + i * HEAD_SIZE
                small = dot(placer, in_f32[:, first : first + HEAD_SIZE].astype(bf16))
                pair_small[i, :, :HEAD_SIZE] = small[:half]
                pair_small[i, :, HEAD_SIZE:] = small[half:]
            own = slice(g * HEAD_SIZE, (g + 1) * HEAD_SIZE)
            pair_small[2, :, :HEAD_SIZE] = value_scale[:half, own]
            pair_small[2, :, HEAD_SIZE:] = value_scale[half:, own]
        if g == 0:
            with phase("fetch"):
                fetches[0].wait()
                fetches[1].wait()
        for sub in range(SUBS):
            with phase("attend"):
                attend(g, sub)
            for j in range(1, inner):
                if is_sided(g):

                    @pl.when(at_end)
                    def _():
                        side_first(g, sub, j).start()

                    @pl.when(jnp.logical_not(at_end))
                    def _():
                        across_copy(g, sub, z, j).start()

                else:
                    across_copy(g, sub, z, j).start()
            for i in range(outer - 1):
                targets = [far[t][i] for t in range(outer)]
                target = pick(targets, z)

                @pl.when(pick([int(is_near(t, o, outer)) for t, o in enumerate(targets)], z) == 1)
                def _():
                    near_copy(g, sub, target).start()

    with phase("selector"):
        lane_r = iota((rows, META), 1)
        line_r = iota((rows, META), 0)
        for i in range(dp):
            fact_row = fact_rows[i]
            owner_in = jnp.sum(
                jnp.where(lane_r == FIRST + line_r, fact_row, 0.0), axis=1, keepdims=True
            )
            line_in = jnp.sum(
                jnp.where(lane_r == FIRST + rows + line_r, fact_row, 0.0), axis=1, keepdims=True
            )
            selector[i * rows : (i + 1) * rows, :] = jnp.where(
                owner_in * slots + line_in == iota((rows, dp * slots), 1).astype(f32), 1.0, 0.0
            ).astype(bf16)

    def side_copy(g, sub, j):
        at = z * inner + lax.rem(y + j, inner)
        return pltpu.make_async_remote_copy(
            src_ref=context.at[g, at, sub],
            dst_ref=context.at[g, at, sub],
            send_sem=local_sem.at[5],
            recv_sem=across_recv.at[g],
            device_id=(beside * inner + y, part),
            device_id_type=MESH,
        )

    order = arrival_order(outer)

    def forward(events, end):
        for _, r, c in events:
            g, sub = chunks[c]
            if r < 0:
                for j in range(1, inner):
                    side_arrival(g, sub, j).wait_recv()
                    side_copy(g, sub, j).start()
                continue
            sources = [order[t][r] for t in range(outer)]
            source = pick(sources, z)
            along_arrival(g, sub, source).wait_recv()

            @pl.when(pick([int(relays(t, o, outer)) for t, o in enumerate(sources)], z) == 1)
            def _():
                relay_copy(g, sub, source).start()

            if is_sided(g) and not end:

                @pl.when(jnp.logical_not(fed & (source == beside)))
                def _():
                    for j in range(1, inner):
                        across_copy(g, sub, source, j).start()

            else:
                for j in range(1, inner):
                    across_copy(g, sub, source, j).start()

    def schedule(lags, side_lag):
        lag = [lags[min(r, len(lags) - 1)] for r in range(outer - 1)]
        side = [
            (c + side_lag, -1, c) for c, (g, _) in enumerate(chunks) if side_lag > 0 and is_sided(g)
        ]
        return sorted([(c + lag[r], r, c) for c in range(len(chunks)) for r in range(outer - 1)] + side)

    with phase("forward"):

        @pl.when(at_end)
        def _():
            forward(schedule(END_LAG, END_SIDE), True)

        @pl.when(jnp.logical_not(at_end))
        def _():
            forward(schedule(MID_LAG, 0.0), False)

    pltpu.make_async_copy(weight, weight, local_sem.at[2]).wait()

    def arrange(g):
        blocks_of = context[g].reshape(dp * slots, group_width)
        return dot(selector[...], blocks_of).astype(bf16)

    def product(arranged, g, n):
        found = dot(arranged, weight[n, g * group_width : (g + 1) * group_width, :])
        return found.reshape(dp, rows, width)

    for g in range(groups - 1):
        with phase("across"):
            across_done(g)
        with phase("product"):
            arranged = arrange(g)
            for n in range(2):
                found = product(arranged, g, n)
                total[n] = found if g == 0 else total[n] + found
    with phase("across"):
        across_done(groups - 1)

    partner = part + 1 - 2 * parity
    swap = pltpu.make_async_remote_copy(
        src_ref=give,
        dst_ref=take,
        send_sem=local_sem.at[6],
        recv_sem=last_recv.at[0],
        device_id=(me, partner),
        device_id_type=MESH,
    )
    with phase("product"):
        arranged = arrange(groups - 1)
        given = product(arranged, groups - 1, 0)
        give[...] = (given if groups == 1 else given + total[0]).astype(bf16)
    swap.start()
    with phase("product"):
        kept = product(arranged, groups - 1, 1)
        total[1] = kept if groups == 1 else kept + total[1]
    with phase("swap"):
        swap.wait_recv()

    target_part = me // blocks
    place = lax.rem(me, blocks) * mp + part

    def part_target(i, j):
        return pick([far[t][i] for t in range(outer)], z) * inner + lax.rem(y + j, inner)

    def part_copy(i, j):
        target = part_target(i, j)
        return pltpu.make_async_remote_copy(
            src_ref=send_part.at[target],
            dst_ref=recv_part.at[place],
            send_sem=local_sem.at[7],
            recv_sem=last_recv.at[1],
            device_id=(target, target_part),
            device_id_type=MESH,
        )
    def parts_wait(buffer, count, semaphore):
        slab = buffer.at[pl.ds(0, count)]
        pltpu.make_async_copy(slab, slab, semaphore).wait()

    with phase("parts"):
        for i, j in sends + [(outer - 1, 0)]:
            target = part_target(i, j)
            send_part[target] = (total[1, target] + take[target].astype(f32)).astype(bf16)
            if (i, j) in sends:
                part_copy(i, j).start()

        @pl.when(target_part != part)
        def _():
            part_copy(outer - 1, 0).start()

        @pl.when(target_part == part)
        def _():
            recv_part[place] = send_part[me]

        @pl.when(target_part != part)
        def _():
            parts_wait(recv_part, dp, last_recv.at[1])

        @pl.when(target_part == part)
        def _():
            parts_wait(recv_part, dp - 1, last_recv.at[1])

    with phase("sum"):
        for e in range(blocks):
            for n in range(2):
                summed = recv_part[e * mp + n].astype(f32)
                for j in range(n + 2, mp, 2):
                    summed = summed + recv_part[e * mp + j].astype(f32)
                first = e * columns + n * width
                out_ref[:, first : first + width] = summed.astype(bf16)

    with phase("drain"):
        slab = send_rows.at[pl.ds(0, dp - 1)]
        pltpu.make_async_copy(slab, slab, local_sem.at[3]).wait()
        for t in range(outer):
            near = sum(is_near(t, s, outer) for s in range(outer) if s != t)
            relayed = sum(relays(t, s, outer) for s in range(outer))

            @pl.when(z == t)
            def _():
                slab = context.at[:, pl.ds(0, near + relayed)]
                pltpu.make_async_copy(slab, slab, local_sem.at[4]).wait()

        for g in range(groups):

            def drain(sources):
                slab = context.at[g, pl.ds(0, sources * (inner - 1))]
                pltpu.make_async_copy(slab, slab, local_sem.at[5]).wait()

            if not is_sided(g):
                drain(outer)
                continue

            for more, role in ((1, at_end), (-1, fed), (0, jnp.logical_not(at_end | fed))):

                @pl.when(role)
                def _():
                    drain(outer + more)

        swap.wait_send()

        @pl.when(target_part != part)
        def _():
            parts_wait(send_part, dp, local_sem.at[7])

        @pl.when(target_part == part)
        def _():
            parts_wait(send_part, dp - 1, local_sem.at[7])


def on_device(
    dp,
    mp,
    queries,
    incoming_key,
    incoming_value,
    key_cache,
    cached_values,
    task_key_scale,
    task_value_scale,
    out_weight,
    task_id,
    cached_length,
    task_owner,
    cache_slot,
):
    rows, query_width = queries.shape
    kv_width = incoming_key.shape[1]
    slots, positions, _ = key_cache.shape
    capacity = 2 * rows // dp
    items = dp * capacity
    columns = out_weight.shape[1]
    row_width = query_width + 2 * kv_width + META
    groups = kv_width // HEAD_SIZE
    group_width = GROUP * HEAD_SIZE
    half = slots // 2
    per = half // SUBS
    outer, inner = factors(dp)
    away = pl.BlockSpec(memory_space=pl.ANY)
    small = [
        queries,
        incoming_key,
        incoming_value,
        task_key_scale,
        task_value_scale,
        task_id.reshape(1, -1),
        cached_length.reshape(1, -1),
        cache_slot.reshape(1, -1),
        task_owner.reshape(1, -1),
    ]
    return pl.pallas_call(
        functools.partial(layer_kernel, dp, mp),
        out_shape=pltpu.VMEM((rows, dp * columns // mp), bf16),
        in_specs=[away] * 12,
        out_specs=pl.BlockSpec(memory_space=pltpu.VMEM),
        scratch_shapes=[pltpu.VMEM(a.shape, a.dtype) for a in small]
        + [
            pltpu.VMEM(key_cache.shape, bf16),
            pltpu.VMEM(cached_values.shape, bf16),
            pltpu.VMEM((2, out_weight.shape[0], columns // 2), bf16),
            pltpu.VMEM((items, row_width), f32),
            pltpu.VMEM((items, row_width), f32),
            pltpu.VMEM((dp, 1, META), f32),
            pltpu.VMEM((dp, capacity, row_width), bf16),
            pltpu.VMEM((dp, capacity, row_width), bf16),
            pltpu.VMEM((half, 2 * GROUP, 2 * HEAD_SIZE), f32),
            pltpu.VMEM((3, half, 2 * HEAD_SIZE), f32),
            pltpu.VMEM((slots, kv_width), f32),
            pltpu.VMEM((slots, positions), f32),
            pltpu.VMEM((per, 2 * GROUP, HEAD_SIZE), f32),
            pltpu.VMEM((groups, dp, SUBS, 2 * per, group_width), bf16),
            pltpu.VMEM((dp * rows, dp * slots), bf16),
            pltpu.VMEM((2, dp, rows, columns // 2), f32),
            pltpu.VMEM((dp, rows, columns // 2), bf16),
            pltpu.VMEM((dp, rows, columns // 2), bf16),
            pltpu.VMEM((dp, rows, columns // 2), bf16),
            pltpu.VMEM((dp, rows, columns // 2), bf16),
            pltpu.SemaphoreType.DMA((len(small),)),
            pltpu.SemaphoreType.DMA((groups,)),
            pltpu.SemaphoreType.DMA((outer - 1, groups, SUBS)),
            pltpu.SemaphoreType.DMA((groups,)),
            pltpu.SemaphoreType.DMA((groups, SUBS, inner - 1)),
            pltpu.SemaphoreType.DMA((2,)),
        ],
        compiler_params=pltpu.CompilerParams(
            collective_id=0, has_side_effects=True, vmem_limit_bytes=60 * 1024 * 1024
        ),
    )(*small, key_cache, cached_values, out_weight)


def solution(mesh):
    placed = (
        P("dp", "mp"),
        P("dp", "mp"),
        P("dp", "mp"),
        P("dp", None, "mp"),
        P("dp", None, "mp"),
        P(None, "mp"),
        P(None, "mp"),
        P("mp", "dp"),
        P("dp"),
        P("dp"),
        P(),
        P("dp"),
    )
    return jax.shard_map(
        functools.partial(on_device, mesh.shape["dp"], mesh.shape["mp"]),
        mesh=mesh,
        in_specs=placed,
        out_specs=P("dp", "mp"),
        check_vma=False,
    )
```

```python
import contextlib
import functools
import math

import jax
import jax.numpy as jnp
from jax import lax
from jax.experimental import pallas as pl
from jax.experimental.pallas import tpu as pltpu
from jax.sharding import PartitionSpec as P

KEY_VALUE_HEADS = 8
HEAD_SIZE = 128
QUERY_HEADS = 64
GROUP = QUERY_HEADS // KEY_VALUE_HEADS
META = 128
FIRST = 16
SUBS = 2
SIDE = 2
END_SIDE = 2.3
END_LAG = (0.0, 3.5, 3.6)
MID_LAG = (0.0, 0.1, 0.2)
SCOPES = False
MESH = pl.DeviceIdType.MESH

masked_score = -1e30
f32 = jnp.float32
bf16 = jnp.bfloat16


def phase(name):
    return jax.named_scope(name) if SCOPES else contextlib.nullcontext()


def iota(shape, dim):
    return lax.broadcasted_iota(jnp.int32, shape, dim)


def to_column(row):
    n = row.shape[1]
    eye = iota((n, n), 0) == iota((n, n), 1)
    return jnp.sum(jnp.where(eye, row, 0.0), axis=1, keepdims=True)


def to_row(column):
    n = column.shape[0]
    eye = iota((n, n), 0) == iota((n, n), 1)
    return jnp.sum(jnp.where(eye, column, 0.0), axis=0, keepdims=True)


def factors(dp):
    inner = 2 ** (int(math.log2(dp)) // 2)
    return dp // inner, inner


def dot(a, b):
    return jnp.dot(a, b, preferred_element_type=f32)


def pick(table, index):
    value = table[0]
    for i in range(1, len(table)):
        value = jnp.where(index == i, table[i], value)
    return value


def far_first(count):
    return [sorted(range(count), key=lambda t: -abs(t - z)) for z in range(count)]


def is_near(source, target, count):
    apart = abs(source - target)
    return apart == 1 or (apart == 2 and 0 < target < count - 1)


def relays(z, source, count):
    beyond = z + (1 if z > source else -1)
    return z != source and 0 <= beyond < count and not is_near(source, beyond, count)


def arrival_order(count):
    def rank(z):
        return lambda s: abs(z - s) - (1.5 if relays(z, s, count) else 0.0)

    return [sorted((s for s in range(count) if s != z), key=rank(z)) for z in range(count)]


def layer_kernel(
    dp,
    mp,
    query_hbm,
    new_key_hbm,
    new_value_hbm,
    key_scale_hbm,
    value_scale_hbm,
    task_hbm,
    length_hbm,
    slot_hbm,
    owner_hbm,
    key_hbm,
    value_hbm,
    weight_hbm,
    out_ref,
    query_ref,
    new_key_ref,
    new_value_ref,
    key_scale_ref,
    value_scale_ref,
    task_ref,
    length_ref,
    slot_ref,
    owner_ref,
    keys,
    values,
    weight,
    rows_f32,
    in_f32,
    fact_rows,
    send_rows,
    recv_rows,
    pair_query,
    pair_small,
    value_scale,
    slot_length,
    slot_context,
    context,
    last_context,
    selector,
    total,
    give,
    take,
    send_part,
    recv_part,
    local_sem,
    request_recv,
    along_recv,
    across_recv,
    side_recv,
    last_recv,
):
    me = lax.axis_index("dp")
    part = lax.axis_index("mp")
    rows, query_width = query_ref.shape
    groups = new_key_ref.shape[1] // HEAD_SIZE
    group_width = GROUP * HEAD_SIZE
    segment = group_width + 2 * HEAD_SIZE
    task_total = key_scale_ref.shape[0]
    slots, positions, _ = keys.shape
    capacity = send_rows.shape[1]
    items = dp * capacity
    columns = weight.shape[1]
    blocks = dp // mp
    half = slots // 2
    per = half // SUBS
    outer, inner = factors(dp)
    z, y = me // inner, lax.rem(me, inner)

    barrier = pltpu.get_barrier_semaphore()
    for k in range(1, dp):
        pl.semaphore_signal(
            barrier, inc=1, device_id=(lax.rem(me + k, dp), part), device_id_type=MESH
        )
    for k in range(1, mp):
        pl.semaphore_signal(
            barrier, inc=1, device_id=(me, lax.rem(part + k, mp)), device_id_type=MESH
        )

    pairs = [
        (task_hbm, task_ref),
        (owner_hbm, owner_ref),
        (length_hbm, length_ref),
        (slot_hbm, slot_ref),
        (key_scale_hbm, key_scale_ref),
        (query_hbm, query_ref),
        (new_key_hbm, new_key_ref),
        (new_value_hbm, new_value_ref),
        (value_scale_hbm, value_scale_ref),
    ]
    inputs = [pltpu.make_async_copy(a, b, local_sem.at[i]) for i, (a, b) in enumerate(pairs)]
    for copy in inputs:
        copy.start()
    parity = lax.rem(part, 2)
    width = columns // 2
    fetches = [
        pltpu.make_async_copy(key_hbm, keys, local_sem.at[0]),
        pltpu.make_async_copy(value_hbm, values, local_sem.at[1]),
        pltpu.make_async_copy(weight_hbm, weight, local_sem.at[2]),
    ]
    pair_query[...] = jnp.zeros_like(pair_query)

    def start_of(g):
        return g * segment + (META if g > 0 else 0)

    def span_of(g):
        return slice(start_of(g), start_of(g) + segment + (META if g == 0 else 0))

    meta = slice(segment, segment + META)

    with phase("inputs"):
        for copy in inputs[:4]:
            copy.wait()
    with phase("pack0"):
        task_column = to_column(task_ref[...].astype(f32))
        length_column = to_column(length_ref[...].astype(f32))
        slot_column = to_column(slot_ref[...].astype(f32))
        picked = task_column == iota((rows, task_total), 1).astype(f32)
        owner_column = jnp.sum(
            jnp.where(picked, owner_ref[...].astype(f32), 0.0), axis=1, keepdims=True
        )
        owner_row = to_row(owner_column)
        earlier = iota((rows, rows), 1) < iota((rows, rows), 0)
        rank = jnp.sum(
            jnp.where(earlier & (owner_column == owner_row), 1.0, 0.0), axis=1, keepdims=True
        )
        position_row = to_row(owner_column * capacity + rank)
        packer = jnp.where(
            position_row == iota((items, rows), 0).astype(f32), 1.0, 0.0
        ).astype(bf16)
        side = jnp.floor(slot_column * (1.0 / half))
        pair = slot_column - side * half
        sub = jnp.floor(pair * (1.0 / per))
        line_column = sub * (2 * per) + side * per + (pair - sub * per)
        lane = iota((rows, META), 1)
        line = iota((rows, META), 0)
        task_high = jnp.floor(task_column * (1.0 / 128.0))
        task_low = task_column - task_high * 128.0
        facts = (
            jnp.where(lane == 0, slot_column + 1.0, 0.0)
            + jnp.where(lane == 1, length_column, 0.0)
            + jnp.where(lane == 2, task_high, 0.0)
            + jnp.where(lane == 3, task_low, 0.0)
        )
        shared = jnp.sum(
            jnp.where(lane == FIRST + line, owner_column, 0.0)
            + jnp.where(lane == FIRST + rows + line, line_column, 0.0),
            axis=0,
            keepdims=True,
        )
        rows_f32[:, meta] = dot(packer, facts.astype(bf16)) + shared
        for copy in inputs[4:]:
            copy.wait()
        for fetch in fetches:
            fetch.start()
        key_factor = dot(jnp.where(picked, 1.0, 0.0).astype(bf16), key_scale_ref[...])

    def pack(g):
        own = slice(g * HEAD_SIZE, (g + 1) * HEAD_SIZE)
        at = start_of(g)
        for h in range(GROUP):
            lanes = slice((g * GROUP + h) * HEAD_SIZE, (g * GROUP + h + 1) * HEAD_SIZE)
            scaled = (query_ref[:, lanes].astype(f32) * key_factor[:, own]).astype(bf16)
            rows_f32[:, at + h * HEAD_SIZE : at + (h + 1) * HEAD_SIZE] = dot(packer, scaled)
        first = key_at(g)
        rows_f32[:, first : first + HEAD_SIZE] = dot(packer, new_key_ref[:, own])
        rows_f32[:, first + HEAD_SIZE : first + 2 * HEAD_SIZE] = dot(packer, new_value_ref[:, own])
        for d in range(dp):
            send_rows[d, :, span_of(g)] = rows_f32[
                d * capacity : (d + 1) * capacity, span_of(g)
            ].astype(bf16)

    def key_at(g):
        return start_of(g) + group_width

    far = far_first(outer)
    sends = [(i, j) for i in range(outer) for j in range(inner - 1, -1, -1)][:-1]

    def request_copy(g, i, j):
        target = pick([far[t][i] for t in range(outer)], z) * inner + lax.rem(y + j, inner)
        return pltpu.make_async_remote_copy(
            src_ref=send_rows.at[target, :, span_of(g)],
            dst_ref=recv_rows.at[me, :, span_of(g)],
            send_sem=local_sem.at[3],
            recv_sem=request_recv.at[g],
            device_id=(target, part),
            device_id_type=MESH,
        )

    def requests_done(g):
        slab = recv_rows.at[pl.ds(0, dp - 1), :, span_of(g)]
        return pltpu.make_async_copy(slab, slab, request_recv.at[g])

    with phase("pack1"):
        pack(0)
    with phase("barrier"):
        pl.semaphore_wait(barrier, dp + mp - 2)
    for g in range(groups):
        if g > 0:
            with phase("pack2"):
                pack(g)
        for i, j in sends:
            request_copy(g, i, j).start()
    recv_rows[me] = send_rows[me]

    inv_root = 1.0 / math.sqrt(HEAD_SIZE)
    key_line = iota((2 * GROUP, positions), 1).astype(f32)
    low_line = iota((2 * GROUP, positions), 0) < GROUP

    def attend(g, sub):
        own = slice(g * HEAD_SIZE, (g + 1) * HEAD_SIZE)
        picks = [sub * per + i for i in range(per)]

        def both(ref, p):
            return jnp.concatenate([ref[p, :, own], ref[p + half, :, own]], axis=1)

        scores, owns, weights, own_weights, tops, shows, sees = [], [], [], [], [], [], []
        for p in picks:
            scores.append(
                lax.dot_general(
                    pair_query[p].astype(bf16),
                    both(keys, p),
                    (((1,), (1,)), ((), ())),
                    preferred_element_type=f32,
                )
                * inv_root
            )
        for p in picks:
            owns.append(
                jnp.sum(pair_query[p] * pair_small[0, p : p + 1, :], axis=1, keepdims=True)
                * inv_root
            )
        for i, p in enumerate(picks):
            length = jnp.where(
                low_line, slot_length[p : p + 1, :], slot_length[p + half : p + half + 1, :]
            )
            sees.append(key_line < length)
            shows.append(jnp.where(sees[i], scores[i], masked_score))
            tops.append(jnp.maximum(jnp.max(shows[i], axis=1, keepdims=True), owns[i]))
        for i in range(per):
            weights.append(jnp.where(sees[i], jnp.exp(shows[i] - tops[i]), 0.0))
            own_weights.append(jnp.exp(owns[i] - tops[i]))
        blends = [dot(weights[i].astype(bf16), both(values, p)) for i, p in enumerate(picks)]
        for i, p in enumerate(picks):
            weight_sum = jnp.sum(weights[i], axis=1, keepdims=True) + own_weights[i]
            one = slice(p, p + 1)
            blended = blends[i] + own_weights[i].astype(bf16).astype(f32) * pair_small[1, one, :]
            attended = (blended / weight_sum).astype(bf16).astype(f32) * pair_small[2, one, :]
            slot_context[i, :GROUP, :] = attended[:GROUP, :HEAD_SIZE]
            slot_context[i, GROUP:, :] = attended[GROUP:, HEAD_SIZE:]
        for h in range(GROUP):
            found = jnp.concatenate(
                [slot_context[:, h, :], slot_context[:, GROUP + h, :]], axis=0
            ).astype(bf16)
            if g < groups - 1:
                context[g, me, sub, :, h * HEAD_SIZE : (h + 1) * HEAD_SIZE] = found
            else:
                piece, at = divmod(h, GROUP // SUBS)
                last_context[
                    me,
                    piece,
                    sub * 2 * per : (sub + 1) * 2 * per,
                    at * HEAD_SIZE : (at + 1) * HEAD_SIZE,
                ] = found

    def chunk_at(g, at, sub):
        return context.at[g, at, sub] if g < groups - 1 else last_context.at[at, sub]

    def near_copy(g, sub, target):
        return pltpu.make_async_remote_copy(
            src_ref=chunk_at(g, me, sub),
            dst_ref=chunk_at(g, me, sub),
            send_sem=local_sem.at[4],
            recv_sem=along_recv.at[z - jnp.where(z > target, 1, 0), g, sub],
            device_id=(target * inner + y, part),
            device_id_type=MESH,
        )

    def along_arrival(g, sub, source):
        at = source * inner + y
        return pltpu.make_async_remote_copy(
            src_ref=chunk_at(g, at, sub),
            dst_ref=chunk_at(g, at, sub),
            send_sem=local_sem.at[4],
            recv_sem=along_recv.at[source - jnp.where(source > z, 1, 0), g, sub],
            device_id=(at, part),
            device_id_type=MESH,
        )

    def relay_copy(g, sub, source):
        at = source * inner + y
        beyond = z + jnp.where(z > source, 1, -1)
        return pltpu.make_async_remote_copy(
            src_ref=chunk_at(g, at, sub),
            dst_ref=chunk_at(g, at, sub),
            send_sem=local_sem.at[4],
            recv_sem=along_recv.at[source - jnp.where(source > beyond, 1, 0), g, sub],
            device_id=(beyond * inner + y, part),
            device_id_type=MESH,
        )

    def across_copy(g, sub, source, j):
        at = source * inner + y
        return pltpu.make_async_remote_copy(
            src_ref=chunk_at(g, at, sub),
            dst_ref=chunk_at(g, at, sub),
            send_sem=local_sem.at[5],
            recv_sem=across_recv.at[across_at(g, sub)],
            device_id=(z * inner + lax.rem(y + j, inner), part),
            device_id_type=MESH,
        )

    def side_first(g, sub, j):
        at = z * inner + lax.rem(y + j, inner)
        return pltpu.make_async_remote_copy(
            src_ref=chunk_at(g, me, sub),
            dst_ref=chunk_at(g, me, sub),
            send_sem=local_sem.at[5],
            recv_sem=side_recv.at[g, sub, inner - j - 1],
            device_id=(at, part),
            device_id_type=MESH,
        )

    def side_arrival(g, sub, j):
        at = z * inner + lax.rem(y + j, inner)
        return pltpu.make_async_remote_copy(
            src_ref=chunk_at(g, at, sub),
            dst_ref=chunk_at(g, at, sub),
            send_sem=local_sem.at[5],
            recv_sem=side_recv.at[g, sub, j - 1],
            device_id=(at, part),
            device_id_type=MESH,
        )

    def across_at(g, sub):
        return g + sub if g == groups - 1 else g

    def across_done(g, sub):
        def wait(sources):
            count = pl.ds(0, sources * (inner - 1))
            slab = context.at[g, count] if g < groups - 1 else last_context.at[count, sub]
            pltpu.make_async_copy(slab, slab, across_recv.at[across_at(g, sub)]).wait()

        if not is_sided(g):
            wait(outer)
            return

        @pl.when(at_end)
        def _():
            wait(outer - 1)

        @pl.when(jnp.logical_not(at_end))
        def _():
            wait(outer)

    def is_sided(g):
        return g >= groups - SIDE * groups // 4

    at_end = (z == 0) | (z == outer - 1)
    beside = z + 1 - 2 * lax.rem(z, 2)
    fed = (z == 1) | (z == outer - 2)
    chunks = [(g, sub) for g in range(groups) for sub in range(SUBS)]
    def send_own(g, sub):
        for j in range(1, inner):
            if is_sided(g):

                @pl.when(at_end)
                def _():
                    side_first(g, sub, j).start()

                @pl.when(jnp.logical_not(at_end))
                def _():
                    across_copy(g, sub, z, j).start()

            else:
                across_copy(g, sub, z, j).start()
        for i in range(outer - 1):
            targets = [far[t][i] for t in range(outer)]
            target = pick(targets, z)

            @pl.when(pick([int(is_near(t, o, outer)) for t, o in enumerate(targets)], z) == 1)
            def _():
                near_copy(g, sub, target).start()

    for g in range(groups):
        with phase("requests"):
            requests_done(g).wait()
        with phase("place"):
            for s in range(dp):
                in_f32[s * capacity : (s + 1) * capacity, span_of(g)] = recv_rows[
                    s, :, span_of(g)
                ].astype(f32)
            if g == 0:
                facts_in = in_f32[:, meta]
                for s in range(dp):
                    fact_rows[s] = in_f32[s * capacity : s * capacity + 1, meta]
                placing_row = to_row(facts_in[:, 0:1])
                placer = jnp.where(
                    placing_row == iota((slots, items), 0).astype(f32) + 1.0, 1.0, 0.0
                ).astype(bf16)
                slot_facts = dot(placer, facts_in.astype(bf16))
                slot_task = slot_facts[:, 2:3] * 128.0 + slot_facts[:, 3:4]
                value_scale[...] = dot(
                    jnp.where(slot_task == iota((slots, task_total), 1).astype(f32), 1.0, 0.0).astype(bf16),
                    value_scale_ref[...],
                )
                slot_length[...] = jnp.broadcast_to(slot_facts[:, 1:2], (slots, positions))
            at = start_of(g)
            for h in range(GROUP):
                placed = dot(
                    placer, in_f32[:, at + h * HEAD_SIZE : at + (h + 1) * HEAD_SIZE].astype(bf16)
                )
                pair_query[:, h, :HEAD_SIZE] = placed[:half]
                pair_query[:, GROUP + h, HEAD_SIZE:] = placed[half:]
            for i in range(2):
                first = key_at(g) + i * HEAD_SIZE
                small = dot(placer, in_f32[:, first : first + HEAD_SIZE].astype(bf16))
                pair_small[i, :, :HEAD_SIZE] = small[:half]
                pair_small[i, :, HEAD_SIZE:] = small[half:]
            own = slice(g * HEAD_SIZE, (g + 1) * HEAD_SIZE)
            pair_small[2, :, :HEAD_SIZE] = value_scale[:half, own]
            pair_small[2, :, HEAD_SIZE:] = value_scale[half:, own]
        if g == 0:
            with phase("fetch"):
                fetches[0].wait()
                fetches[1].wait()
        for sub in range(SUBS):
            with phase("attend"):
                attend(g, sub)
            if g < groups - 1:
                send_own(g, sub)
        if g == groups - 1:
            for sub in range(SUBS):
                send_own(g, sub)

    with phase("selector"):
        lane_r = iota((rows, META), 1)
        line_r = iota((rows, META), 0)
        for i in range(dp):
            fact_row = fact_rows[i]
            owner_in = jnp.sum(
                jnp.where(lane_r == FIRST + line_r, fact_row, 0.0), axis=1, keepdims=True
            )
            line_in = jnp.sum(
                jnp.where(lane_r == FIRST + rows + line_r, fact_row, 0.0), axis=1, keepdims=True
            )
            selector[i * rows : (i + 1) * rows, :] = jnp.where(
                owner_in * slots + line_in == iota((rows, dp * slots), 1).astype(f32), 1.0, 0.0
            ).astype(bf16)

    def side_copy(g, sub, j):
        at = z * inner + lax.rem(y + j, inner)
        return pltpu.make_async_remote_copy(
            src_ref=chunk_at(g, at, sub),
            dst_ref=chunk_at(g, at, sub),
            send_sem=local_sem.at[5],
            recv_sem=across_recv.at[across_at(g, sub)],
            device_id=(beside * inner + y, part),
            device_id_type=MESH,
        )

    order = arrival_order(outer)

    def forward(events, end):
        for _, r, c in events:
            g, sub = chunks[c]
            if r < 0:
                for j in range(1, inner):
                    side_arrival(g, sub, j).wait_recv()
                    side_copy(g, sub, j).start()
                continue
            sources = [order[t][r] for t in range(outer)]
            source = pick(sources, z)
            along_arrival(g, sub, source).wait_recv()

            @pl.when(pick([int(relays(t, o, outer)) for t, o in enumerate(sources)], z) == 1)
            def _():
                relay_copy(g, sub, source).start()

            if is_sided(g) and not end:

                @pl.when(jnp.logical_not(fed & (source == beside)))
                def _():
                    for j in range(1, inner):
                        across_copy(g, sub, source, j).start()

            else:
                for j in range(1, inner):
                    across_copy(g, sub, source, j).start()

    def schedule(lags, side_lag):
        lag = [lags[min(r, len(lags) - 1)] for r in range(outer - 1)]
        side = [
            (c + side_lag, -1, c) for c, (g, _) in enumerate(chunks) if side_lag > 0 and is_sided(g)
        ]
        return sorted([(c + lag[r], r, c) for c in range(len(chunks)) for r in range(outer - 1)] + side)

    with phase("forward"):

        @pl.when(at_end)
        def _():
            forward(schedule(END_LAG, END_SIDE), True)

        @pl.when(jnp.logical_not(at_end))
        def _():
            forward(schedule(MID_LAG, 0.0), False)

    fetches[2].wait()

    piece_width = group_width // SUBS

    def product(contexts, first):
        wide = contexts.shape[-1]
        arranged = dot(selector[...], contexts.reshape(dp * slots, wide)).astype(bf16)
        return [
            dot(
                arranged, weight[first : first + wide, n * width : (n + 1) * width]
            ).reshape(dp, rows, width)
            for n in range(2)
        ]

    def add(found, started):
        for n in range(2):
            total[n] = total[n] + found[n] if started else found[n]

    for g in range(groups - 1):
        with phase("across"):
            across_done(g, 0)
        with phase("product"):
            add(product(context[g], g * group_width), g > 0)
    last_first = (groups - 1) * group_width
    for sub in range(SUBS - 1):
        with phase("across"):
            across_done(groups - 1, sub)
        with phase("product"):
            add(
                product(last_context[:, sub], last_first + sub * piece_width),
                groups > 1 or sub > 0,
            )
    with phase("across"):
        across_done(groups - 1, SUBS - 1)

    partner = part + 1 - 2 * parity

    def swap(n):
        return pltpu.make_async_remote_copy(
            src_ref=give.at[n],
            dst_ref=take.at[n],
            send_sem=local_sem.at[6],
            recv_sem=last_recv.at[0],
            device_id=(me, partner),
            device_id_type=MESH,
        )

    middle = dp // 2
    kept_at = parity * middle
    given_at = middle - kept_at
    with phase("product"):
        found = product(last_context[:, SUBS - 1], last_first + (SUBS - 1) * piece_width)
        for n in range(2):
            total[n] = total[n] + found[n]
            give[n] = total[n, pl.ds(given_at, middle)].astype(bf16)
            swap(n).start()
    with phase("swap"):
        pltpu.make_async_copy(take, take, last_recv.at[0]).wait()

    target_part = me // blocks
    lanes_of = mp // 2
    place = lax.rem(me, blocks) * lanes_of + part // 2
    stays = (target_part == part) & (me // middle == parity)

    def part_copy(at):
        return pltpu.make_async_remote_copy(
            src_ref=send_part.at[at],
            dst_ref=recv_part.at[place],
            send_sem=local_sem.at[7],
            recv_sem=last_recv.at[1],
            device_id=(kept_at + at, target_part),
            device_id_type=MESH,
        )

    def parts_wait(buffer, count, semaphore):
        slab = buffer.at[pl.ds(0, count)]
        pltpu.make_async_copy(slab, slab, semaphore).wait()

    with phase("parts"):
        for at in range(middle):
            for n in range(2):
                send_part[at, :, n * width : (n + 1) * width] = (
                    total[n, kept_at + at] + take[n, at].astype(f32)
                ).astype(bf16)
            own = stays & (kept_at + at == me)

            @pl.when(jnp.logical_not(own))
            def _():
                part_copy(at).start()

        @pl.when(stays)
        def _():
            recv_part[place] = send_part[me - kept_at]
            parts_wait(recv_part, blocks * lanes_of - 1, last_recv.at[1])

        @pl.when(jnp.logical_not(stays))
        def _():
            parts_wait(recv_part, blocks * lanes_of, last_recv.at[1])

    with phase("sum"):
        for e in range(blocks):
            summed = recv_part[e * lanes_of].astype(f32)
            for j in range(1, lanes_of):
                summed = summed + recv_part[e * lanes_of + j].astype(f32)
            out_ref[:, e * columns : (e + 1) * columns] = summed.astype(bf16)

    with phase("drain"):
        slab = send_rows.at[pl.ds(0, dp - 1)]
        pltpu.make_async_copy(slab, slab, local_sem.at[3]).wait()
        for t in range(outer):
            near = sum(is_near(t, s, outer) for s in range(outer) if s != t)
            relayed = sum(relays(t, s, outer) for s in range(outer))

            @pl.when(z == t)
            def _():
                slab = last_context.at[pl.ds(0, (near + relayed) * groups)]
                pltpu.make_async_copy(slab, slab, local_sem.at[4]).wait()

        for g in range(groups):

            def drain(sources):
                slab = last_context.at[pl.ds(0, sources * (inner - 1))]
                pltpu.make_async_copy(slab, slab, local_sem.at[5]).wait()

            if not is_sided(g):
                drain(outer)
                continue

            for more, role in ((1, at_end), (-1, fed), (0, jnp.logical_not(at_end | fed))):

                @pl.when(role)
                def _():
                    drain(outer + more)

        pltpu.make_async_copy(give, give, local_sem.at[6]).wait()

        @pl.when(stays)
        def _():
            parts_wait(send_part, middle - 1, local_sem.at[7])

        @pl.when(jnp.logical_not(stays))
        def _():
            parts_wait(send_part, middle, local_sem.at[7])


def on_device(
    dp,
    mp,
    queries,
    incoming_key,
    incoming_value,
    key_cache,
    cached_values,
    task_key_scale,
    task_value_scale,
    out_weight,
    task_id,
    cached_length,
    task_owner,
    cache_slot,
):
    rows, query_width = queries.shape
    kv_width = incoming_key.shape[1]
    slots, positions, _ = key_cache.shape
    capacity = 2 * rows // dp
    items = dp * capacity
    columns = out_weight.shape[1]
    row_width = query_width + 2 * kv_width + META
    groups = kv_width // HEAD_SIZE
    group_width = GROUP * HEAD_SIZE
    half = slots // 2
    per = half // SUBS
    outer, inner = factors(dp)
    away = pl.BlockSpec(memory_space=pl.ANY)
    small = [
        queries,
        incoming_key,
        incoming_value,
        task_key_scale,
        task_value_scale,
        task_id.reshape(1, -1),
        cached_length.reshape(1, -1),
        cache_slot.reshape(1, -1),
        task_owner.reshape(1, -1),
    ]
    return pl.pallas_call(
        functools.partial(layer_kernel, dp, mp),
        out_shape=pltpu.VMEM((rows, dp * columns // mp), bf16),
        in_specs=[away] * 12,
        out_specs=pl.BlockSpec(memory_space=pltpu.VMEM),
        scratch_shapes=[pltpu.VMEM(a.shape, a.dtype) for a in small]
        + [
            pltpu.VMEM(key_cache.shape, bf16),
            pltpu.VMEM(cached_values.shape, bf16),
            pltpu.VMEM(out_weight.shape, bf16),
            pltpu.VMEM((items, row_width), f32),
            pltpu.VMEM((items, row_width), f32),
            pltpu.VMEM((dp, 1, META), f32),
            pltpu.VMEM((dp, capacity, row_width), bf16),
            pltpu.VMEM((dp, capacity, row_width), bf16),
            pltpu.VMEM((half, 2 * GROUP, 2 * HEAD_SIZE), f32),
            pltpu.VMEM((3, half, 2 * HEAD_SIZE), f32),
            pltpu.VMEM((slots, kv_width), f32),
            pltpu.VMEM((slots, positions), f32),
            pltpu.VMEM((per, 2 * GROUP, HEAD_SIZE), f32),
            pltpu.VMEM((max(groups - 1, 1), dp, SUBS, 2 * per, group_width), bf16),
            pltpu.VMEM((dp, SUBS, slots, group_width // SUBS), bf16),
            pltpu.VMEM((dp * rows, dp * slots), bf16),
            pltpu.VMEM((2, dp, rows, columns // 2), f32),
            pltpu.VMEM((2, dp // 2, rows, columns // 2), bf16),
            pltpu.VMEM((2, dp // 2, rows, columns // 2), bf16),
            pltpu.VMEM((dp // 2, rows, columns), bf16),
            pltpu.VMEM((dp // 2, rows, columns), bf16),
            pltpu.SemaphoreType.DMA((len(small),)),
            pltpu.SemaphoreType.DMA((groups,)),
            pltpu.SemaphoreType.DMA((outer - 1, groups, SUBS)),
            pltpu.SemaphoreType.DMA((groups - 1 + SUBS,)),
            pltpu.SemaphoreType.DMA((groups, SUBS, inner - 1)),
            pltpu.SemaphoreType.DMA((2,)),
        ],
        compiler_params=pltpu.CompilerParams(
            collective_id=0, has_side_effects=True, vmem_limit_bytes=60 * 1024 * 1024
        ),
    )(*small, key_cache, cached_values, out_weight)


def solution(mesh):
    placed = (
        P("dp", "mp"),
        P("dp", "mp"),
        P("dp", "mp"),
        P("dp", None, "mp"),
        P("dp", None, "mp"),
        P(None, "mp"),
        P(None, "mp"),
        P("mp", "dp"),
        P("dp"),
        P("dp"),
        P(),
        P("dp"),
    )
    return jax.shard_map(
        functools.partial(on_device, mesh.shape["dp"], mesh.shape["mp"]),
        mesh=mesh,
        in_specs=placed,
        out_specs=P("dp", "mp"),
        check_vma=False,
    )
```

```python
import contextlib
import functools
import math

import jax
import jax.numpy as jnp
from jax import lax
from jax.experimental import pallas as pl
from jax.experimental.pallas import tpu as pltpu
from jax.sharding import PartitionSpec as P

KEY_VALUE_HEADS = 8
HEAD_SIZE = 128
QUERY_HEADS = 64
GROUP = QUERY_HEADS // KEY_VALUE_HEADS
META = 128
FIRST = 16
SUBS = 2
SIDE = 2
END_SIDE = 2.3
END_LAG = (0.0, 3.5, 3.6)
MID_LAG = (0.0, 0.1, 0.2)
SCOPES = False
MESH = pl.DeviceIdType.MESH

masked_score = -1e30
f32 = jnp.float32
bf16 = jnp.bfloat16


def phase(name):
    return jax.named_scope(name) if SCOPES else contextlib.nullcontext()


def iota(shape, dim):
    return lax.broadcasted_iota(jnp.int32, shape, dim)


def to_column(row):
    n = row.shape[1]
    eye = iota((n, n), 0) == iota((n, n), 1)
    return jnp.sum(jnp.where(eye, row, 0.0), axis=1, keepdims=True)


def to_row(column):
    n = column.shape[0]
    eye = iota((n, n), 0) == iota((n, n), 1)
    return jnp.sum(jnp.where(eye, column, 0.0), axis=0, keepdims=True)


def factors(dp):
    inner = 2 ** (int(math.log2(dp)) // 2)
    return dp // inner, inner


def dot(a, b):
    return jnp.dot(a, b, preferred_element_type=f32)


def pick(table, index):
    value = table[0]
    for i in range(1, len(table)):
        value = jnp.where(index == i, table[i], value)
    return value


def far_first(count):
    return [sorted(range(count), key=lambda t: -abs(t - z)) for z in range(count)]


def is_near(source, target, count):
    apart = abs(source - target)
    return apart == 1 or (apart == 2 and 0 < target < count - 1)


def relays(z, source, count):
    beyond = z + (1 if z > source else -1)
    return z != source and 0 <= beyond < count and not is_near(source, beyond, count)


def arrival_order(count):
    def rank(z):
        return lambda s: abs(z - s) - (1.5 if relays(z, s, count) else 0.0)

    return [sorted((s for s in range(count) if s != z), key=rank(z)) for z in range(count)]


def layer_kernel(
    dp,
    mp,
    query_hbm,
    new_key_hbm,
    new_value_hbm,
    key_scale_hbm,
    value_scale_hbm,
    task_hbm,
    length_hbm,
    slot_hbm,
    owner_hbm,
    key_hbm,
    value_hbm,
    weight_hbm,
    out_ref,
    query_ref,
    new_key_ref,
    new_value_ref,
    key_scale_ref,
    value_scale_ref,
    task_ref,
    length_ref,
    slot_ref,
    owner_ref,
    keys,
    values,
    weight,
    rows_f32,
    in_f32,
    fact_rows,
    send_rows,
    recv_rows,
    pair_query,
    pair_small,
    value_scale,
    slot_length,
    slot_context,
    context,
    last_context,
    selector,
    total,
    give,
    take,
    send_part,
    recv_part,
    local_sem,
    request_recv,
    along_recv,
    across_recv,
    side_recv,
    last_recv,
):
    me = lax.axis_index("dp")
    part = lax.axis_index("mp")
    rows, query_width = query_ref.shape
    groups = new_key_ref.shape[1] // HEAD_SIZE
    group_width = GROUP * HEAD_SIZE
    segment = group_width + 2 * HEAD_SIZE
    task_total = key_scale_ref.shape[0]
    slots, positions, _ = keys.shape
    capacity = send_rows.shape[1]
    items = dp * capacity
    columns = weight.shape[1]
    blocks = dp // mp
    half = slots // 2
    per = half // SUBS
    outer, inner = factors(dp)
    z, y = me // inner, lax.rem(me, inner)

    barrier = pltpu.get_barrier_semaphore()
    for k in range(1, dp):
        pl.semaphore_signal(
            barrier, inc=1, device_id=(lax.rem(me + k, dp), part), device_id_type=MESH
        )
    for k in range(1, mp):
        pl.semaphore_signal(
            barrier, inc=1, device_id=(me, lax.rem(part + k, mp)), device_id_type=MESH
        )

    pairs = [
        (task_hbm, task_ref),
        (owner_hbm, owner_ref),
        (length_hbm, length_ref),
        (slot_hbm, slot_ref),
        (key_scale_hbm, key_scale_ref),
        (query_hbm, query_ref),
        (new_key_hbm, new_key_ref),
        (new_value_hbm, new_value_ref),
    ]
    inputs = [pltpu.make_async_copy(a, b, local_sem.at[i]) for i, (a, b) in enumerate(pairs)]
    for copy in inputs:
        copy.start()
    parity = lax.rem(part, 2)
    width = columns // 2
    scale_fetch = pltpu.make_async_copy(value_scale_hbm, value_scale_ref, local_sem.at[6])
    fetches = [
        pltpu.make_async_copy(key_hbm, keys, local_sem.at[0]),
        pltpu.make_async_copy(value_hbm, values, local_sem.at[1]),
        pltpu.make_async_copy(weight_hbm, weight, local_sem.at[2]),
    ]
    pair_query[...] = jnp.zeros_like(pair_query)

    def start_of(g):
        return g * segment + (META if g > 0 else 0)

    def span_of(g):
        return slice(start_of(g), start_of(g) + segment + (META if g == 0 else 0))

    meta = slice(segment, segment + META)

    with phase("inputs"):
        for copy in inputs[:4]:
            copy.wait()
    with phase("pack0"):
        task_column = to_column(task_ref[...].astype(f32))
        length_column = to_column(length_ref[...].astype(f32))
        slot_column = to_column(slot_ref[...].astype(f32))
        picked = task_column == iota((rows, task_total), 1).astype(f32)
        owner_column = jnp.sum(
            jnp.where(picked, owner_ref[...].astype(f32), 0.0), axis=1, keepdims=True
        )
        owner_row = to_row(owner_column)
        earlier = iota((rows, rows), 1) < iota((rows, rows), 0)
        rank = jnp.sum(
            jnp.where(earlier & (owner_column == owner_row), 1.0, 0.0), axis=1, keepdims=True
        )
        position_row = to_row(owner_column * capacity + rank)
        packer = jnp.where(
            position_row == iota((items, rows), 0).astype(f32), 1.0, 0.0
        ).astype(bf16)
        side = jnp.floor(slot_column * (1.0 / half))
        pair = slot_column - side * half
        sub = jnp.floor(pair * (1.0 / per))
        line_column = sub * (2 * per) + side * per + (pair - sub * per)
        lane = iota((rows, META), 1)
        line = iota((rows, META), 0)
        task_high = jnp.floor(task_column * (1.0 / 128.0))
        task_low = task_column - task_high * 128.0
        facts = (
            jnp.where(lane == 0, slot_column + 1.0, 0.0)
            + jnp.where(lane == 1, length_column, 0.0)
            + jnp.where(lane == 2, task_high, 0.0)
            + jnp.where(lane == 3, task_low, 0.0)
        )
        shared = jnp.sum(
            jnp.where(lane == FIRST + line, owner_column, 0.0)
            + jnp.where(lane == FIRST + rows + line, line_column, 0.0),
            axis=0,
            keepdims=True,
        )
        rows_f32[:, meta] = dot(packer, facts.astype(bf16)) + shared
        for copy in inputs[4:]:
            copy.wait()
        scale_fetch.start()
        for fetch in fetches:
            fetch.start()
        key_factor = dot(jnp.where(picked, 1.0, 0.0).astype(bf16), key_scale_ref[...])

    def pack(g):
        own = slice(g * HEAD_SIZE, (g + 1) * HEAD_SIZE)
        at = start_of(g)
        for h in range(GROUP):
            lanes = slice((g * GROUP + h) * HEAD_SIZE, (g * GROUP + h + 1) * HEAD_SIZE)
            scaled = (query_ref[:, lanes].astype(f32) * key_factor[:, own]).astype(bf16)
            rows_f32[:, at + h * HEAD_SIZE : at + (h + 1) * HEAD_SIZE] = dot(packer, scaled)
        first = key_at(g)
        rows_f32[:, first : first + HEAD_SIZE] = dot(packer, new_key_ref[:, own])
        rows_f32[:, first + HEAD_SIZE : first + 2 * HEAD_SIZE] = dot(packer, new_value_ref[:, own])
        for d in range(dp):
            send_rows[d, :, span_of(g)] = rows_f32[
                d * capacity : (d + 1) * capacity, span_of(g)
            ].astype(bf16)

    def key_at(g):
        return start_of(g) + group_width

    far = far_first(outer)
    sends = [(i, j) for i in range(outer) for j in range(inner - 1, -1, -1)][:-1]

    def request_copy(g, i, j):
        target = pick([far[t][i] for t in range(outer)], z) * inner + lax.rem(y + j, inner)
        return pltpu.make_async_remote_copy(
            src_ref=send_rows.at[target, :, span_of(g)],
            dst_ref=recv_rows.at[me, :, span_of(g)],
            send_sem=local_sem.at[3],
            recv_sem=request_recv.at[g],
            device_id=(target, part),
            device_id_type=MESH,
        )

    def requests_done(g):
        slab = recv_rows.at[pl.ds(0, dp - 1), :, span_of(g)]
        return pltpu.make_async_copy(slab, slab, request_recv.at[g])

    with phase("pack1"):
        pack(0)
    with phase("barrier"):
        pl.semaphore_wait(barrier, dp + mp - 2)
    for g in range(groups):
        if g > 0:
            with phase("pack2"):
                pack(g)
        for i, j in sends:
            request_copy(g, i, j).start()
    recv_rows[me] = send_rows[me]

    inv_root = 1.0 / math.sqrt(HEAD_SIZE)
    key_line = iota((2 * GROUP, positions), 1).astype(f32)
    low_line = iota((2 * GROUP, positions), 0) < GROUP

    def attend(g, sub):
        own = slice(g * HEAD_SIZE, (g + 1) * HEAD_SIZE)
        picks = [sub * per + i for i in range(per)]

        def both(ref, p):
            return jnp.concatenate([ref[p, :, own], ref[p + half, :, own]], axis=1)

        scores, owns, weights, own_weights, tops, shows, sees = [], [], [], [], [], [], []
        for p in picks:
            scores.append(
                lax.dot_general(
                    pair_query[p].astype(bf16),
                    both(keys, p),
                    (((1,), (1,)), ((), ())),
                    preferred_element_type=f32,
                )
                * inv_root
            )
        for p in picks:
            owns.append(
                jnp.sum(pair_query[p] * pair_small[0, p : p + 1, :], axis=1, keepdims=True)
                * inv_root
            )
        for i, p in enumerate(picks):
            length = jnp.where(
                low_line, slot_length[p : p + 1, :], slot_length[p + half : p + half + 1, :]
            )
            sees.append(key_line < length)
            shows.append(jnp.where(sees[i], scores[i], masked_score))
            tops.append(jnp.maximum(jnp.max(shows[i], axis=1, keepdims=True), owns[i]))
        for i in range(per):
            weights.append(jnp.where(sees[i], jnp.exp(shows[i] - tops[i]), 0.0))
            own_weights.append(jnp.exp(owns[i] - tops[i]))
        blends = [dot(weights[i].astype(bf16), both(values, p)) for i, p in enumerate(picks)]
        for i, p in enumerate(picks):
            weight_sum = jnp.sum(weights[i], axis=1, keepdims=True) + own_weights[i]
            one = slice(p, p + 1)
            blended = blends[i] + own_weights[i].astype(bf16).astype(f32) * pair_small[1, one, :]
            attended = (blended / weight_sum).astype(bf16).astype(f32) * pair_small[2, one, :]
            slot_context[i, :GROUP, :] = attended[:GROUP, :HEAD_SIZE]
            slot_context[i, GROUP:, :] = attended[GROUP:, HEAD_SIZE:]
        for h in range(GROUP):
            found = jnp.concatenate(
                [slot_context[:, h, :], slot_context[:, GROUP + h, :]], axis=0
            ).astype(bf16)
            if g < groups - 1:
                context[g, me, sub, :, h * HEAD_SIZE : (h + 1) * HEAD_SIZE] = found
            else:
                piece, at = divmod(h, GROUP // SUBS)
                last_context[
                    me,
                    piece,
                    sub * 2 * per : (sub + 1) * 2 * per,
                    at * HEAD_SIZE : (at + 1) * HEAD_SIZE,
                ] = found

    def chunk_at(g, at, sub):
        return context.at[g, at, sub] if g < groups - 1 else last_context.at[at, sub]

    def near_copy(g, sub, target):
        return pltpu.make_async_remote_copy(
            src_ref=chunk_at(g, me, sub),
            dst_ref=chunk_at(g, me, sub),
            send_sem=local_sem.at[4],
            recv_sem=along_recv.at[z - jnp.where(z > target, 1, 0), g, sub],
            device_id=(target * inner + y, part),
            device_id_type=MESH,
        )

    def along_arrival(g, sub, source):
        at = source * inner + y
        return pltpu.make_async_remote_copy(
            src_ref=chunk_at(g, at, sub),
            dst_ref=chunk_at(g, at, sub),
            send_sem=local_sem.at[4],
            recv_sem=along_recv.at[source - jnp.where(source > z, 1, 0), g, sub],
            device_id=(at, part),
            device_id_type=MESH,
        )

    def relay_copy(g, sub, source):
        at = source * inner + y
        beyond = z + jnp.where(z > source, 1, -1)
        return pltpu.make_async_remote_copy(
            src_ref=chunk_at(g, at, sub),
            dst_ref=chunk_at(g, at, sub),
            send_sem=local_sem.at[4],
            recv_sem=along_recv.at[source - jnp.where(source > beyond, 1, 0), g, sub],
            device_id=(beyond * inner + y, part),
            device_id_type=MESH,
        )

    def across_copy(g, sub, source, j):
        at = source * inner + y
        return pltpu.make_async_remote_copy(
            src_ref=chunk_at(g, at, sub),
            dst_ref=chunk_at(g, at, sub),
            send_sem=local_sem.at[5],
            recv_sem=across_recv.at[across_at(g, sub)],
            device_id=(z * inner + lax.rem(y + j, inner), part),
            device_id_type=MESH,
        )

    def side_first(g, sub, j):
        at = z * inner + lax.rem(y + j, inner)
        return pltpu.make_async_remote_copy(
            src_ref=chunk_at(g, me, sub),
            dst_ref=chunk_at(g, me, sub),
            send_sem=local_sem.at[5],
            recv_sem=side_recv.at[groups - 1 - g, sub, inner - j - 1],
            device_id=(at, part),
            device_id_type=MESH,
        )

    def side_arrival(g, sub, j):
        at = z * inner + lax.rem(y + j, inner)
        return pltpu.make_async_remote_copy(
            src_ref=chunk_at(g, at, sub),
            dst_ref=chunk_at(g, at, sub),
            send_sem=local_sem.at[5],
            recv_sem=side_recv.at[groups - 1 - g, sub, j - 1],
            device_id=(at, part),
            device_id_type=MESH,
        )

    def across_at(g, sub):
        return g + sub if g == groups - 1 else g

    def across_done(g, sub):
        def wait(sources):
            count = pl.ds(0, sources * (inner - 1))
            slab = context.at[g, count] if g < groups - 1 else last_context.at[count, sub]
            pltpu.make_async_copy(slab, slab, across_recv.at[across_at(g, sub)]).wait()

        if not is_sided(g):
            wait(outer)
            return

        @pl.when(at_end)
        def _():
            wait(outer - 1)

        @pl.when(jnp.logical_not(at_end))
        def _():
            wait(outer)

    def is_sided(g):
        return g >= groups - SIDE * groups // 4

    at_end = (z == 0) | (z == outer - 1)
    beside = z + 1 - 2 * lax.rem(z, 2)
    fed = (z == 1) | (z == outer - 2)
    chunks = [(g, sub) for g in range(groups) for sub in range(SUBS)]
    def send_own(g, sub):
        for j in range(1, inner):
            if is_sided(g):

                @pl.when(at_end)
                def _():
                    side_first(g, sub, j).start()

                @pl.when(jnp.logical_not(at_end))
                def _():
                    across_copy(g, sub, z, j).start()

            else:
                across_copy(g, sub, z, j).start()
        for i in range(outer - 1):
            targets = [far[t][i] for t in range(outer)]
            target = pick(targets, z)

            @pl.when(pick([int(is_near(t, o, outer)) for t, o in enumerate(targets)], z) == 1)
            def _():
                near_copy(g, sub, target).start()

    for g in range(groups):
        with phase("requests"):
            requests_done(g).wait()
        if g == 0:
            scale_fetch.wait()
        with phase("place"):
            for s in range(dp):
                in_f32[s * capacity : (s + 1) * capacity, span_of(g)] = recv_rows[
                    s, :, span_of(g)
                ].astype(f32)
            if g == 0:
                facts_in = in_f32[:, meta]
                for s in range(dp):
                    fact_rows[s] = in_f32[s * capacity : s * capacity + 1, meta]
                placing_row = to_row(facts_in[:, 0:1])
                placer = jnp.where(
                    placing_row == iota((slots, items), 0).astype(f32) + 1.0, 1.0, 0.0
                ).astype(bf16)
                slot_facts = dot(placer, facts_in.astype(bf16))
                slot_task = slot_facts[:, 2:3] * 128.0 + slot_facts[:, 3:4]
                value_scale[...] = dot(
                    jnp.where(slot_task == iota((slots, task_total), 1).astype(f32), 1.0, 0.0).astype(bf16),
                    value_scale_ref[...],
                )
                slot_length[...] = jnp.broadcast_to(slot_facts[:, 1:2], (slots, positions))
            at = start_of(g)
            for h in range(GROUP):
                placed = dot(
                    placer, in_f32[:, at + h * HEAD_SIZE : at + (h + 1) * HEAD_SIZE].astype(bf16)
                )
                pair_query[:, h, :HEAD_SIZE] = placed[:half]
                pair_query[:, GROUP + h, HEAD_SIZE:] = placed[half:]
            for i in range(2):
                first = key_at(g) + i * HEAD_SIZE
                small = dot(placer, in_f32[:, first : first + HEAD_SIZE].astype(bf16))
                pair_small[i, :, :HEAD_SIZE] = small[:half]
                pair_small[i, :, HEAD_SIZE:] = small[half:]
            own = slice(g * HEAD_SIZE, (g + 1) * HEAD_SIZE)
            pair_small[2, :, :HEAD_SIZE] = value_scale[:half, own]
            pair_small[2, :, HEAD_SIZE:] = value_scale[half:, own]
        if g == 0:
            with phase("fetch"):
                fetches[0].wait()
                fetches[1].wait()
        for sub in range(SUBS):
            with phase("attend"):
                attend(g, sub)
            if g < groups - 1:
                send_own(g, sub)
        if g == groups - 1:
            for sub in range(SUBS):
                send_own(g, sub)

    with phase("selector"):
        lane_r = iota((rows, META), 1)
        line_r = iota((rows, META), 0)
        for i in range(dp):
            fact_row = fact_rows[i]
            owner_in = jnp.sum(
                jnp.where(lane_r == FIRST + line_r, fact_row, 0.0), axis=1, keepdims=True
            )
            line_in = jnp.sum(
                jnp.where(lane_r == FIRST + rows + line_r, fact_row, 0.0), axis=1, keepdims=True
            )
            selector[i * rows : (i + 1) * rows, :] = jnp.where(
                owner_in * slots + line_in == iota((rows, dp * slots), 1).astype(f32), 1.0, 0.0
            ).astype(bf16)

    def side_copy(g, sub, j):
        at = z * inner + lax.rem(y + j, inner)
        return pltpu.make_async_remote_copy(
            src_ref=chunk_at(g, at, sub),
            dst_ref=chunk_at(g, at, sub),
            send_sem=local_sem.at[5],
            recv_sem=across_recv.at[across_at(g, sub)],
            device_id=(beside * inner + y, part),
            device_id_type=MESH,
        )

    order = arrival_order(outer)

    def forward(events, end):
        for _, r, c in events:
            g, sub = chunks[c]
            if r < 0:
                for j in range(1, inner):
                    side_arrival(g, sub, j).wait_recv()
                    side_copy(g, sub, j).start()
                continue
            sources = [order[t][r] for t in range(outer)]
            source = pick(sources, z)
            along_arrival(g, sub, source).wait_recv()

            @pl.when(pick([int(relays(t, o, outer)) for t, o in enumerate(sources)], z) == 1)
            def _():
                relay_copy(g, sub, source).start()

            if is_sided(g) and not end:

                @pl.when(jnp.logical_not(fed & (source == beside)))
                def _():
                    for j in range(1, inner):
                        across_copy(g, sub, source, j).start()

            else:
                for j in range(1, inner):
                    across_copy(g, sub, source, j).start()

    def schedule(lags, side_lag):
        lag = [lags[min(r, len(lags) - 1)] for r in range(outer - 1)]
        side = [
            (c + side_lag, -1, c) for c, (g, _) in enumerate(chunks) if side_lag > 0 and is_sided(g)
        ]
        return sorted([(c + lag[r], r, c) for c in range(len(chunks)) for r in range(outer - 1)] + side)

    with phase("forward"):

        @pl.when(at_end)
        def _():
            forward(schedule(END_LAG, END_SIDE), True)

        @pl.when(jnp.logical_not(at_end))
        def _():
            forward(schedule(MID_LAG, 0.0), False)

    fetches[2].wait()

    piece_width = group_width // SUBS

    def product(contexts, first):
        wide = contexts.shape[-1]
        arranged = dot(selector[...], contexts.reshape(dp * slots, wide)).astype(bf16)
        return [
            dot(
                arranged, weight[first : first + wide, n * width : (n + 1) * width]
            ).reshape(dp, rows, width)
            for n in range(2)
        ]

    def add(found, started):
        for n in range(2):
            total[n] = total[n] + found[n] if started else found[n]

    for g in range(groups - 1):
        with phase("across"):
            across_done(g, 0)
        with phase("product"):
            add(product(context[g], g * group_width), g > 0)
    last_first = (groups - 1) * group_width
    for sub in range(SUBS - 1):
        with phase("across"):
            across_done(groups - 1, sub)
        with phase("product"):
            add(
                product(last_context[:, sub], last_first + sub * piece_width),
                groups > 1 or sub > 0,
            )
    with phase("across"):
        across_done(groups - 1, SUBS - 1)

    partner = part + 1 - 2 * parity

    def swap(n):
        return pltpu.make_async_remote_copy(
            src_ref=give.at[n],
            dst_ref=take.at[n],
            send_sem=local_sem.at[6],
            recv_sem=last_recv.at[0],
            device_id=(me, partner),
            device_id_type=MESH,
        )

    middle = dp // 2
    kept_at = parity * middle
    given_at = middle - kept_at
    with phase("product"):
        found = product(last_context[:, SUBS - 1], last_first + (SUBS - 1) * piece_width)
        for n in range(2):
            total[n] = total[n] + found[n]
            give[n] = total[n, pl.ds(given_at, middle)].astype(bf16)
            swap(n).start()
    with phase("swap"):
        pltpu.make_async_copy(take, take, last_recv.at[0]).wait()

    target_part = me // blocks
    lanes_of = mp // 2
    place = lax.rem(me, blocks) * lanes_of + part // 2
    stays = (target_part == part) & (me // middle == parity)

    def part_copy(at):
        return pltpu.make_async_remote_copy(
            src_ref=send_part.at[at],
            dst_ref=recv_part.at[place],
            send_sem=local_sem.at[7],
            recv_sem=last_recv.at[1],
            device_id=(kept_at + at, target_part),
            device_id_type=MESH,
        )

    def parts_wait(buffer, count, semaphore):
        slab = buffer.at[pl.ds(0, count)]
        pltpu.make_async_copy(slab, slab, semaphore).wait()

    with phase("parts"):
        for at in range(middle):
            for n in range(2):
                send_part[at, :, n * width : (n + 1) * width] = (
                    total[n, kept_at + at] + take[n, at].astype(f32)
                ).astype(bf16)
            own = stays & (kept_at + at == me)

            @pl.when(jnp.logical_not(own))
            def _():
                part_copy(at).start()

        @pl.when(stays)
        def _():
            recv_part[place] = send_part[me - kept_at]
            parts_wait(recv_part, blocks * lanes_of - 1, last_recv.at[1])

        @pl.when(jnp.logical_not(stays))
        def _():
            parts_wait(recv_part, blocks * lanes_of, last_recv.at[1])

    with phase("sum"):
        for e in range(blocks):
            summed = recv_part[e * lanes_of].astype(f32)
            for j in range(1, lanes_of):
                summed = summed + recv_part[e * lanes_of + j].astype(f32)
            out_ref[:, e * columns : (e + 1) * columns] = summed.astype(bf16)

    with phase("drain"):
        slab = send_rows.at[pl.ds(0, dp - 1)]
        pltpu.make_async_copy(slab, slab, local_sem.at[3]).wait()
        for t in range(outer):
            near = sum(is_near(t, s, outer) for s in range(outer) if s != t)
            relayed = sum(relays(t, s, outer) for s in range(outer))

            @pl.when(z == t)
            def _():
                slab = last_context.at[pl.ds(0, (near + relayed) * groups)]
                pltpu.make_async_copy(slab, slab, local_sem.at[4]).wait()

        for g in range(groups):

            def drain(sources):
                slab = last_context.at[pl.ds(0, sources * (inner - 1))]
                pltpu.make_async_copy(slab, slab, local_sem.at[5]).wait()

            if not is_sided(g):
                drain(outer)
                continue

            for more, role in ((1, at_end), (-1, fed), (0, jnp.logical_not(at_end | fed))):

                @pl.when(role)
                def _():
                    drain(outer + more)

        pltpu.make_async_copy(give, give, local_sem.at[6]).wait()

        @pl.when(stays)
        def _():
            parts_wait(send_part, middle - 1, local_sem.at[7])

        @pl.when(jnp.logical_not(stays))
        def _():
            parts_wait(send_part, middle, local_sem.at[7])


def on_device(
    dp,
    mp,
    queries,
    incoming_key,
    incoming_value,
    key_cache,
    cached_values,
    task_key_scale,
    task_value_scale,
    out_weight,
    task_id,
    cached_length,
    task_owner,
    cache_slot,
):
    rows, query_width = queries.shape
    kv_width = incoming_key.shape[1]
    slots, positions, _ = key_cache.shape
    capacity = 2 * rows // dp
    items = dp * capacity
    columns = out_weight.shape[1]
    row_width = query_width + 2 * kv_width + META
    groups = kv_width // HEAD_SIZE
    group_width = GROUP * HEAD_SIZE
    half = slots // 2
    per = half // SUBS
    outer, inner = factors(dp)
    away = pl.BlockSpec(memory_space=pl.ANY)
    small = [
        queries,
        incoming_key,
        incoming_value,
        task_key_scale,
        task_value_scale,
        task_id.reshape(1, -1),
        cached_length.reshape(1, -1),
        cache_slot.reshape(1, -1),
        task_owner.reshape(1, -1),
    ]
    return pl.pallas_call(
        functools.partial(layer_kernel, dp, mp),
        out_shape=pltpu.VMEM((rows, dp * columns // mp), bf16),
        in_specs=[away] * 12,
        out_specs=pl.BlockSpec(memory_space=pltpu.VMEM),
        scratch_shapes=[pltpu.VMEM(a.shape, a.dtype) for a in small]
        + [
            pltpu.VMEM(key_cache.shape, bf16),
            pltpu.VMEM(cached_values.shape, bf16),
            pltpu.VMEM(out_weight.shape, bf16),
            pltpu.VMEM((items, row_width), f32),
            pltpu.VMEM((items, row_width), f32),
            pltpu.VMEM((dp, 1, META), f32),
            pltpu.VMEM((dp, capacity, row_width), bf16),
            pltpu.VMEM((dp, capacity, row_width), bf16),
            pltpu.VMEM((half, 2 * GROUP, 2 * HEAD_SIZE), f32),
            pltpu.VMEM((3, half, 2 * HEAD_SIZE), f32),
            pltpu.VMEM((slots, kv_width), f32),
            pltpu.VMEM((slots, positions), f32),
            pltpu.VMEM((per, 2 * GROUP, HEAD_SIZE), f32),
            pltpu.VMEM((max(groups - 1, 1), dp, SUBS, 2 * per, group_width), bf16),
            pltpu.VMEM((dp, SUBS, slots, group_width // SUBS), bf16),
            pltpu.VMEM((dp * rows, dp * slots), bf16),
            pltpu.VMEM((2, dp, rows, columns // 2), f32),
            pltpu.VMEM((2, dp // 2, rows, columns // 2), bf16),
            pltpu.VMEM((2, dp // 2, rows, columns // 2), bf16),
            pltpu.VMEM((dp // 2, rows, columns), bf16),
            pltpu.VMEM((dp // 2, rows, columns), bf16),
            pltpu.SemaphoreType.DMA((len(small) - 1,)),
            pltpu.SemaphoreType.DMA((groups,)),
            pltpu.SemaphoreType.DMA((outer - 1, groups, SUBS)),
            pltpu.SemaphoreType.DMA((groups - 1 + SUBS,)),
            pltpu.SemaphoreType.DMA((max(SIDE * groups // 4, 1), SUBS, inner - 1)),
            pltpu.SemaphoreType.DMA((2,)),
        ],
        compiler_params=pltpu.CompilerParams(
            collective_id=0, has_side_effects=True, vmem_limit_bytes=60 * 1024 * 1024
        ),
    )(*small, key_cache, cached_values, out_weight)


def solution(mesh):
    placed = (
        P("dp", "mp"),
        P("dp", "mp"),
        P("dp", "mp"),
        P("dp", None, "mp"),
        P("dp", None, "mp"),
        P(None, "mp"),
        P(None, "mp"),
        P("mp", "dp"),
        P("dp"),
        P("dp"),
        P(),
        P("dp"),
    )
    return jax.shard_map(
        functools.partial(on_device, mesh.shape["dp"], mesh.shape["mp"]),
        mesh=mesh,
        in_specs=placed,
        out_specs=P("dp", "mp"),
        check_vma=False,
    )
```
